32 devices in a mesh: pipe: 2 (over y), dp: 4 (over z), tensor: 4 (over x, core).
Axes of the slice: x: 2, y: 2, z: 4, core: 2. Of those that a mesh axis runs over, the one named last changes fastest.
Arguments:
- saved: bfloat16 [2, 2, 256, 1024], P('pipe', None, 'dp'), may hold values from -6 to 6
- top_grad: bfloat16 [2, 256, 1024], P(None, 'dp'), may hold values from -6 to 6
- gain: bfloat16 [2, 1024], P('pipe', 'dp'), may hold values from 0.25 to 1.75
- w_query: bfloat16 [2, 1024, 1536], P('pipe', 'dp', 'tensor'), may hold values from -0.1875 to 0.1875
- w_latent: bfloat16 [2, 1024, 576], P('pipe', 'dp'), may hold values from -0.1875 to 0.1875
- compressed_gain: bfloat16 [2, 512], P('pipe', 'dp'), may hold values from 0.25 to 1.75
- expand_weight: bfloat16 [2, 512, 2048], P('pipe', 'dp', 'tensor'), may hold values from -0.25 to 0.25
- w_output: bfloat16 [2, 1024, 1024], P('pipe', 'tensor', 'dp'), may hold values from -0.1875 to 0.1875
Outputs:
- input_grad: bfloat16 [2, 2, 256, 1024], P('pipe', None, ('dp', 'tensor'))
- grad_gain: float32 [2, 1024], P('pipe', 'dp')
- grad_query: float32 [2, 1024, 1536], P('pipe', 'dp', 'tensor')
- grad_latent: float32 [2, 1024, 576], P('pipe', 'dp')
- grad_latent_gain: float32 [2, 512], P('pipe', 'dp')
- grad_expand: float32 [2, 512, 2048], P('pipe', 'dp', 'tensor')
- grad_output: float32 [2, 1024, 1024], P('pipe', 'tensor', 'dp')
The draws below stay inside these ranges and needn't reach their ends.
All inputs are finite; a program needn't handle non-finite values.
Results may differ from the reference program's by a relative error of at most 0.04.
Values may be sent and summed in bfloat16 or wider, within the bound.
No kernel may reach another device: no remote copies, remote signals or barrier semaphores. Data moves between devices by JAX's collectives and lax.ppermute only.
A program may use at most 64 MiB of HBM per device.

```python
import jax
import jax.numpy as jnp
from jax import lax

MODEL_WIDTH = 1024
NOPE = 128
ROPE = 64
VDIM = 128
COMPRESSED_RANK = 512
MB = 2
MB_TOK = 64
SECTION_COUNT = 2
TOKENS = 256
QUERY_COLUMNS = 1536
LATENT_COLUMNS = 576
EXPAND_COLUMNS = 2048
OUTPUT_ROWS = 1024
N_DP = 4
N_TENSOR = 4


def steps_of(rng, dims, pieces, low, top_value):
    def one(position, blocks):
        heights = jax.random.uniform(jax.random.fold_in(jax.random.fold_in(rng, 6), position), (blocks,), jnp.float32, low / len(pieces), top_value / len(pieces))
        return jnp.repeat(jnp.exp(heights), dims[position] // blocks).reshape((-1,) + (1,) * (len(dims) - position - 1))

    level = one(*pieces[0])
    for cut in pieces[1:]:
        level = level * one(*cut)
    return level


def normal_values(rng, dims, deviation, bound, shards=(), kind=jnp.bfloat16):
    array = jax.random.normal(rng, dims, jnp.float32) * deviation
    if len(shards) > 0:
        array = steps_of(rng, dims, shards, -0.22, 0.18) * array
    return jnp.clip(array, min=-bound, max=bound).astype(kind)


def setup_inputs(seed: int = 0) -> dict:
    seeds = jax.random.split(jax.random.key(seed), 9)
    return {
        "saved": normal_values(seeds[0], (SECTION_COUNT, MB, TOKENS, MODEL_WIDTH), 1.0, 6.0, ((0, 2), (2, 4))),
        "top_grad": normal_values(seeds[1], (MB, TOKENS, MODEL_WIDTH), 1.0, 6.0, ((1, 4),)),
        "gain": jnp.clip(1.0 + 0.15 * jax.random.normal(seeds[2], (SECTION_COUNT, MODEL_WIDTH), jnp.float32), 0.25, 1.75).astype(jnp.bfloat16),
        "w_query": normal_values(seeds[3], (SECTION_COUNT, MODEL_WIDTH, QUERY_COLUMNS), MODEL_WIDTH ** -0.5, 0.1875, ((0, 2), (1, 4), (2, 4))),
        "w_latent": normal_values(seeds[4], (SECTION_COUNT, MODEL_WIDTH, LATENT_COLUMNS), MODEL_WIDTH ** -0.5, 0.1875, ((0, 2), (1, 4))),
        "compressed_gain": jnp.clip(1.0 + 0.15 * jax.random.normal(seeds[5], (SECTION_COUNT, COMPRESSED_RANK), jnp.float32), 0.25, 1.75).astype(jnp.bfloat16),
        "expand_weight": normal_values(seeds[6], (SECTION_COUNT, COMPRESSED_RANK, EXPAND_COLUMNS), COMPRESSED_RANK ** -0.5, 0.25, ((0, 2), (1, 4), (2, 4))),
        "w_output": normal_values(seeds[7], (SECTION_COUNT, OUTPUT_ROWS, MODEL_WIDTH), OUTPUT_ROWS ** -0.5, 0.1875, ((0, 2), (1, 4), (2, 4))),
    }


EPS = 1e-06

def root_mean_scale(values, scale):
    return values * lax.rsqrt(lax.optimization_barrier(jnp.mean(values * values, axis=-1, keepdims=True)) + EPS) * scale

def rotary_angles(values):
    length = values.shape[0]
    half = values.shape[-1] // 2
    freq = jnp.exp(-jnp.log(10000.0) * jnp.arange(half, dtype=jnp.float32) / half)
    angle = jnp.arange(length, dtype=jnp.float32)[:, None] * freq[None, :]
    cosine = jnp.cos(angle)[:, None, :]
    sine = jnp.sin(angle)[:, None, :]
    first = values[..., :half]
    second = values[..., half:]
    return jnp.concatenate([first * cosine - second * sine, second * cosine + first * sine], axis=-1)

def branch(normed, w_q, w_lat, latent_norm_gain, w_exp, w_out):
    length = normed.shape[0]
    heads = w_q.shape[1] // (NOPE + ROPE)
    rounded = normed.astype(jnp.bfloat16)
    query = jnp.dot(rounded, w_q, preferred_element_type=jnp.float32).reshape(length, heads, NOPE + ROPE)
    latent_state = jnp.dot(rounded, w_lat, preferred_element_type=jnp.float32)
    compressed_state = root_mean_scale(latent_state[:, :COMPRESSED_RANK], latent_norm_gain).astype(jnp.bfloat16)
    rotary_key_part = rotary_angles(latent_state[:, None, COMPRESSED_RANK:])[:, 0, :]
    expanded = jnp.dot(compressed_state, w_exp, preferred_element_type=jnp.float32).reshape(length, heads, NOPE + VDIM)
    key_nope = expanded[:, :, :NOPE]
    values = expanded[:, :, NOPE:].astype(jnp.bfloat16)
    query_rope = rotary_angles(query[:, :, NOPE:])
    scores = jnp.einsum('qhd,khd->hqk', query[:, :, :NOPE], key_nope) + jnp.einsum('qhd,kd->hqk', query_rope, rotary_key_part)
    scores = scores * (NOPE + ROPE) ** (-0.5)
    causal = jnp.arange(length)[:, None] >= jnp.arange(length)[None, :]
    scores = jnp.where(causal[None], scores, -1e+30)
    weights = jax.nn.softmax(scores, axis=-1).astype(jnp.bfloat16)
    mixed = jnp.einsum('hqk,khd->qhd', weights.astype(jnp.float32), values.astype(jnp.float32))
    mixed = mixed.astype(jnp.bfloat16).reshape(length, heads * VDIM)
    return jnp.dot(mixed, w_out, preferred_element_type=jnp.float32)

def reference(saved, top_grad, gain, w_query, w_latent, compressed_gain, expand_weight, w_output):
    head_groups = N_TENSOR
    dgrads = []
    all_input = []
    upstream = top_grad
    for section_index in reversed(range(SECTION_COUNT)):
        gain32 = gain[section_index].astype(jnp.float32)
        lgain32 = compressed_gain[section_index].astype(jnp.float32)
        lat_w = w_latent[section_index]
        q_groups = w_query[section_index].reshape(MODEL_WIDTH, head_groups, QUERY_COLUMNS // head_groups).transpose(1, 0, 2)
        expand_groups = expand_weight[section_index].reshape(COMPRESSED_RANK, head_groups, EXPAND_COLUMNS // head_groups).transpose(1, 0, 2)
        o_groups = w_output[section_index].reshape(head_groups, OUTPUT_ROWS // head_groups, MODEL_WIDTH)

        def one_sequence(loop_carry, pair):
            x_rows, up_rows = pair
            normed, norm_pull = jax.vjp(root_mean_scale, x_rows.astype(jnp.float32), gain32)
            cot = up_rows.astype(jnp.float32)

            def one_group(wq_g, we_g, wo_g):
                unused, pull = jax.vjp(branch, normed, wq_g, lat_w, lgain32, we_g, wo_g)
                return pull(cot)
            d_norm, d_q, d_lat, d_lg, expand_gradient, d_o = jax.vmap(one_group)(q_groups, expand_groups, o_groups)
            d_normed = lax.optimization_barrier(jnp.sum(d_norm, axis=0))
            dx_norm, d_gain = norm_pull(d_normed)
            dx = (cot + dx_norm).astype(jnp.bfloat16)
            g_q = d_q.astype(jnp.float32).transpose(1, 0, 2).reshape(MODEL_WIDTH, QUERY_COLUMNS)
            expand_weight_grad = expand_gradient.astype(jnp.float32).transpose(1, 0, 2).reshape(COMPRESSED_RANK, EXPAND_COLUMNS)
            g_o = d_o.astype(jnp.float32).reshape(OUTPUT_ROWS, MODEL_WIDTH)
            g_lat = lax.optimization_barrier(jnp.sum(d_lat.astype(jnp.float32), axis=0))
            g_lg = lax.optimization_barrier(jnp.sum(d_lg, axis=0))
            loop_carry = (loop_carry[0] + d_gain, loop_carry[1] + g_q, loop_carry[2] + g_lat, loop_carry[3] + g_lg, loop_carry[4] + expand_weight_grad, loop_carry[5] + g_o)
            return (loop_carry, dx)
        loop_carry = (jnp.zeros((MODEL_WIDTH,), jnp.float32), jnp.zeros((MODEL_WIDTH, QUERY_COLUMNS), jnp.float32), jnp.zeros((MODEL_WIDTH, LATENT_COLUMNS), jnp.float32), jnp.zeros((COMPRESSED_RANK,), jnp.float32), jnp.zeros((COMPRESSED_RANK, EXPAND_COLUMNS), jnp.float32), jnp.zeros((OUTPUT_ROWS, MODEL_WIDTH), jnp.float32))
        section_inputs = []
        for micro in range(MB):
            x_seq = saved[section_index, micro].reshape(N_DP, MB_TOK, MODEL_WIDTH)
            up_seq = upstream[micro].reshape(N_DP, MB_TOK, MODEL_WIDTH)
            loop_carry, dx = lax.scan(one_sequence, loop_carry, (x_seq, up_seq))
            section_inputs.append(dx.reshape(TOKENS, MODEL_WIDTH))
        upstream = jnp.stack(section_inputs)
        all_input.append(upstream)
        dgrads.append(loop_carry)
    all_input = all_input[::-1]
    dgrads = dgrads[::-1]
    input_grad = jnp.stack(all_input)
    outs = [jnp.stack([entry[k] for entry in dgrads]) for k in range(6)]
    return (input_grad, outs[0], outs[1], outs[2], outs[3], outs[4], outs[5])
```

```python
import functools

import jax
import jax.numpy as jnp
import numpy as np
from jax import lax
from jax.experimental import pallas as pl
from jax.experimental.pallas import tpu as pltpu
from jax.sharding import PartitionSpec as P

NOPE = 128
ROPE = 64
VDIM = 128
COMPRESSED_RANK = 512


EPS = 1e-06


def passed_along(value, axis, steps):
    count = lax.axis_size(axis)
    first, last = (max(0, -steps), min(count, count - steps))
    return lax.ppermute(value, axis, [(source, source + steps) for source in range(first, last)])


def root_mean_scale(values, scale):
    return values * lax.rsqrt(jnp.mean(values * values, axis=-1, keepdims=True) + EPS) * scale


def rotary_angles(values):
    length = values.shape[0]
    half = values.shape[-1] // 2
    freq = jnp.exp(-jnp.log(10000.0) * jnp.arange(half, dtype=jnp.float32) / half)
    angle = jnp.arange(length, dtype=jnp.float32)[:, None] * freq[None, :]
    cosine = jnp.cos(angle)[:, None, :]
    sine = jnp.sin(angle)[:, None, :]
    first = values[..., :half]
    second = values[..., half:]
    return jnp.concatenate(
        [first * cosine - second * sine, second * cosine + first * sine], axis=-1
    )


def branch(normed, w_q, w_lat, latent_norm_gain, w_exp, w_out):
    length = normed.shape[0]
    heads = w_q.shape[1] // (NOPE + ROPE)
    rounded = normed.astype(jnp.bfloat16)
    query = jnp.dot(rounded, w_q, preferred_element_type=jnp.float32).reshape(
        length, heads, NOPE + ROPE
    )
    latent_state = jnp.dot(rounded, w_lat, preferred_element_type=jnp.float32)
    compressed_state = root_mean_scale(latent_state[:, :COMPRESSED_RANK], latent_norm_gain).astype(
        jnp.bfloat16
    )
    rotary_key_part = rotary_angles(latent_state[:, None, COMPRESSED_RANK:])[:, 0, :]
    expanded = jnp.dot(compressed_state, w_exp, preferred_element_type=jnp.float32).reshape(
        length, heads, NOPE + VDIM
    )
    key_nope = expanded[:, :, :NOPE]
    values = expanded[:, :, NOPE:].astype(jnp.bfloat16)
    query_rope = rotary_angles(query[:, :, NOPE:])
    scores = jnp.einsum("qhd,khd->hqk", query[:, :, :NOPE], key_nope) + jnp.einsum(
        "qhd,kd->hqk", query_rope, rotary_key_part
    )
    scores = scores * (NOPE + ROPE) ** (-0.5)
    causal = jnp.arange(length)[:, None] >= jnp.arange(length)[None, :]
    scores = jnp.where(causal[None], scores, -1e30)
    weights = jax.nn.softmax(scores, axis=-1).astype(jnp.bfloat16)
    mixed = jnp.einsum("hqk,khd->qhd", weights.astype(jnp.float32), values.astype(jnp.float32))
    mixed = mixed.astype(jnp.bfloat16).reshape(length, heads * VDIM)
    return jnp.dot(mixed, w_out, preferred_element_type=jnp.float32)


def plain_shards(saved, top_grad, gain, w_query, w_latent, compressed_gain, expand_weight, w_output):
    gathered = (
        lax.all_gather(gain, "dp", axis=1, tiled=True),
        lax.all_gather(w_query, "dp", axis=1, tiled=True),
        lax.all_gather(w_latent, "dp", axis=1, tiled=True),
        lax.all_gather(compressed_gain, "dp", axis=1, tiled=True),
        lax.all_gather(expand_weight, "dp", axis=1, tiled=True),
        lax.all_gather(w_output, "dp", axis=2, tiled=True),
    )
    gain32 = gathered[0][0].astype(jnp.float32)
    query_all = gathered[1][0]
    latent_all = gathered[2][0]
    lgain32 = gathered[3][0].astype(jnp.float32)
    expand_all = gathered[4][0]
    output_all = gathered[5][0]
    sections = lax.axis_size("pipe")
    section_index = lax.axis_index("pipe")
    tensor_count = lax.axis_size("tensor")
    tensor_rank = lax.axis_index("tensor")
    micro_count = saved.shape[1]
    length = saved.shape[2]
    width = saved.shape[3]
    share = length // tensor_count

    def compute(normed, upstream):
        unused, pull = jax.vjp(
            lambda value: branch(value, query_all, latent_all, lgain32, expand_all, output_all),
            normed,
        )
        return pull(upstream.astype(jnp.float32))[0]

    def skip(normed, upstream):
        return jnp.zeros_like(normed)

    gain_total = jnp.zeros((width,), jnp.float32)
    results = jnp.zeros((micro_count, share, width), jnp.bfloat16)
    stored = jnp.zeros((micro_count, length, width), jnp.bfloat16)
    received = jnp.zeros((length, width), jnp.bfloat16)
    for tick in range(sections + micro_count - 1):
        micro = tick - (sections - 1 - section_index)
        active = jnp.logical_and(micro >= 0, micro < micro_count)
        picked = jnp.clip(micro, 0, micro_count - 1)
        x_rows = lax.dynamic_index_in_dim(saved[0], picked, 0, keepdims=False)
        top_rows = lax.dynamic_index_in_dim(top_grad, picked, 0, keepdims=False)
        arrived = received
        upstream = jnp.where(section_index == sections - 1, top_rows, arrived)
        x_float = x_rows.astype(jnp.float32)
        normed, norm_pull = jax.vjp(root_mean_scale, x_float, gain32)
        branch_grad = lax.cond(active, compute, skip, normed, upstream)
        d_normed = lax.psum(branch_grad.astype(jnp.bfloat16), "tensor").astype(jnp.float32)
        dx_norm, d_gain = norm_pull(d_normed)
        dx = (upstream.astype(jnp.float32) + dx_norm).astype(jnp.bfloat16)
        gain_total = gain_total + jnp.where(active, d_gain, 0.0)
        mine = lax.dynamic_slice_in_dim(dx, tensor_rank * share, share, 0)
        chosen = (jnp.arange(micro_count) == micro)[:, None, None]
        results = jnp.where(chosen, mine[None], results)
        stored = jnp.where(chosen, upstream[None], stored)
        received = passed_along(dx, "pipe", -1)
    totals = (
        jnp.zeros(query_all.shape, jnp.float32),
        jnp.zeros(latent_all.shape, jnp.float32),
        jnp.zeros(lgain32.shape, jnp.float32),
        jnp.zeros(expand_all.shape, jnp.float32),
        jnp.zeros(output_all.shape, jnp.float32),
    )
    for micro_index in range(micro_count):
        normed_again = root_mean_scale(saved[0, micro_index].astype(jnp.float32), gain32)
        unused, weight_pull = jax.vjp(
            lambda w_q, w_lat, lat_gain, w_exp, w_out: branch(
                normed_again, w_q, w_lat, lat_gain, w_exp, w_out
            ),
            query_all,
            latent_all,
            lgain32,
            expand_all,
            output_all,
        )
        cotangents = weight_pull(stored[micro_index].astype(jnp.float32))
        totals = tuple(
            (total + piece.astype(jnp.float32) for total, piece in zip(totals, cotangents))
        )
    gain_part = jnp.where(tensor_rank == 0, gain_total, 0.0)
    grad_q, grad_lat, grad_lg, grad_e, grad_o = totals
    out_q, part_lat, part_lg, out_e, out_o, part_gain = (
        lax.psum_scatter(grad_q.astype(jnp.bfloat16), "dp", scatter_dimension=0, tiled=True).astype(
            jnp.float32
        ),
        lax.psum_scatter(
            grad_lat.astype(jnp.bfloat16), "dp", scatter_dimension=0, tiled=True
        ).astype(jnp.float32),
        lax.psum_scatter(
            grad_lg.astype(jnp.bfloat16), "dp", scatter_dimension=0, tiled=True
        ).astype(jnp.float32),
        lax.psum_scatter(grad_e.astype(jnp.bfloat16), "dp", scatter_dimension=0, tiled=True).astype(
            jnp.float32
        ),
        lax.psum_scatter(grad_o.astype(jnp.bfloat16), "dp", scatter_dimension=1, tiled=True).astype(
            jnp.float32
        ),
        lax.psum_scatter(
            gain_part.astype(jnp.bfloat16), "dp", scatter_dimension=0, tiled=True
        ).astype(jnp.float32),
    )
    out_lat, out_lg, out_gain = (
        lax.psum(part_lat.astype(jnp.bfloat16), "tensor").astype(jnp.float32),
        lax.psum(part_lg.astype(jnp.bfloat16), "tensor").astype(jnp.float32),
        lax.psum(part_gain.astype(jnp.bfloat16), "tensor").astype(jnp.float32),
    )
    return (
        results[None],
        out_gain[None],
        out_q[None],
        out_lat[None],
        out_lg[None],
        out_e[None],
        out_o[None],
    )


F32 = jnp.float32
BF16 = jnp.bfloat16


def mm(a, b):
    return lax.dot_general(a, b, (((1,), (0,)), ((), ())), preferred_element_type=F32)


def mm_nt(a, b):
    return lax.dot_general(a, b, (((1,), (1,)), ((), ())), preferred_element_type=F32)


def mm_tn(a, b):
    return lax.dot_general(a, b, (((0,), (0,)), ((), ())), preferred_element_type=F32)


def turned(values):
    half = values.shape[1] // 2
    return jnp.concatenate([values[:, half:], values[:, :half]], axis=1)


def rotate(values, cosine, sine):
    return values * cosine + turned(values) * sine


def rotate_back(values, cosine, sine):
    return values * cosine - turned(values) * sine


class Plan:
    def __init__(self, saved, w_query, w_latent, expand_weight, w_output, n_pipe, n_dp, n_tensor):
        self.n_pipe, self.n, self.nt = n_pipe, n_dp, n_tensor
        self.micro, self.length, self.width = saved.shape[1:]
        self.rows = self.micro * self.length
        self.share = self.length // n_tensor
        self.heads = w_query.shape[2] // (NOPE + ROPE)
        self.rank = expand_weight.shape[1] * n_dp
        self.latent = w_latent.shape[2]
        self.wcol = self.width // n_dp
        self.ccol = self.rank // n_dp
        self.qcol = self.heads * (NOPE + ROPE)
        self.hcol = self.heads * VDIM
        self.rope_all = self.heads * ROPE
        self.o_comp = self.wcol
        self.o_mixed = self.o_comp + self.ccol
        self.o_q = self.o_mixed + self.hcol
        self.o_kn = self.o_q + self.qcol
        self.o_kr = self.o_kn + self.heads * NOPE
        self.pay = self.o_kr + ROPE
        self.o_dv = self.heads * self.length
        self.o_up = self.o_dv + self.hcol
        self.tail = self.o_up + self.wcol
        self.misc = self.width // self.rank + 1
        self.dl_rows = self.micro * self.share + 16 * ((2 * self.misc + 15) // 16)

    def fits(self):
        aligned = self.wcol % 256 == 0 and self.ccol % 128 == 0 and self.rope_all % 128 == 0
        whole = self.width % self.rank == 0 and (self.heads * self.length) % 128 == 0
        return aligned and whole and self.nt % 2 == 0 and self.share % 16 == 0 and self.rows <= 512


def forward_body(plan, ranks, x, gains, wq, lat_own, lat_other, wexp, cosine, sine, outs):
    (pays, v_ref, p_ref, chat_ref, rc_ref, gain_ref, cgain_ref, x_own, g_s, cg_s, n_s, h_s, c_s) = outs
    n, nt = plan.n, plan.nt
    j, t = ranks[0], ranks[1]
    core = lax.rem(t, 2)
    half = plan.wcol // 2
    for k in range(n):
        src = lax.rem(j - k + n, n)
        g_s[src] = gains[k][:, : plan.wcol].astype(F32)
        cg_s[src] = gains[k][:, plan.wcol :].astype(F32)
    xf = x[...].astype(F32)
    scale = lax.rsqrt(jnp.mean(xf * xf, axis=1, keepdims=True) + EPS)
    for b in range(n):
        block = xf[:, b * plan.wcol : (b + 1) * plan.wcol] * scale * g_s[b]
        rounded = block.astype(BF16)
        n_s[b] = rounded
        h_s[2 * b] = rounded[:, :half]
        h_s[2 * b + 1] = rounded[:, half:]
        gain_ref[:, b * plan.wcol : (b + 1) * plan.wcol] = g_s[b]
        cgain_ref[:, b * plan.ccol : (b + 1) * plan.ccol] = cg_s[b]
    query = jnp.zeros((plan.rows, plan.qcol), F32)
    latent = jnp.zeros((plan.rows, plan.latent), F32)
    for k in range(n):
        src = lax.rem(j - k + n, n)
        query = query + mm(n_s[src], wq[k][...])
        latent = latent + mm(h_s[2 * src + core], lat_own[k][...])
        latent = latent + mm(h_s[2 * src + 1 - core], lat_other[k][...])
    low = latent[:, : plan.rank]
    rc = lax.rsqrt(jnp.mean(low * low, axis=1, keepdims=True) + EPS)
    chat = low * rc
    chat_ref[...] = chat
    rc_ref[...] = rc
    comp = (chat * cgain_ref[...]).astype(BF16)
    for b in range(n):
        c_s[b] = comp[:, b * plan.ccol : (b + 1) * plan.ccol]
    expanded = jnp.zeros((plan.rows, plan.heads * (NOPE + VDIM)), F32)
    for k in range(n):
        src = lax.rem(j - k + n, n)
        expanded = expanded + mm(c_s[src], wexp[k][...])
    cos, sin = cosine[...], sine[...]
    kr = rotate(latent[:, plan.rank :], cos, sin).astype(BF16)
    row = lax.broadcasted_iota(jnp.int32, (plan.rows, plan.rows), 0)
    col = lax.broadcasted_iota(jnp.int32, (plan.rows, plan.rows), 1)
    keep = row >= col
    for m in range(1, plan.micro):
        keep = keep & ((row < m * plan.length) | (col >= m * plan.length))
    qn_all, qr_all, kn_all, mixed_all = [], [], [], []
    for h in range(plan.heads):
        q_at = h * (NOPE + ROPE)
        e_at = h * (NOPE + VDIM)
        qn = query[:, q_at : q_at + NOPE].astype(BF16)
        qr = rotate(query[:, q_at + NOPE : q_at + NOPE + ROPE], cos, sin).astype(BF16)
        kn = expanded[:, e_at : e_at + NOPE].astype(BF16)
        v = expanded[:, e_at + NOPE : e_at + NOPE + VDIM].astype(BF16)
        scores = (mm_nt(qn, kn) + mm_nt(qr, kr)) * (NOPE + ROPE) ** (-0.5)
        scores = jnp.where(keep, scores, -1e30)
        top = jnp.max(scores, axis=1, keepdims=True)
        e = jnp.exp(scores - top)
        p = e / jnp.sum(e, axis=1, keepdims=True)
        p_ref[h] = p
        mixed = mm(p.astype(BF16), v).astype(BF16)
        v_ref[:, h * VDIM : (h + 1) * VDIM] = v
        qn_all.append(qn)
        qr_all.append(qr)
        kn_all.append(kn)
        mixed_all.append(mixed)
    qr_cat = jnp.concatenate(qr_all, axis=1)
    for k in range(n):
        dst = lax.rem(j + k, n)
        pays[k][:, : plan.wcol] = n_s[dst]
        pays[k][:, plan.o_comp : plan.o_mixed] = c_s[dst]
        for h in range(plan.heads):
            pays[k][:, plan.o_mixed + h * VDIM : plan.o_mixed + (h + 1) * VDIM] = mixed_all[h]
            pays[k][:, plan.o_q + h * NOPE : plan.o_q + (h + 1) * NOPE] = qn_all[h]
            pays[k][:, plan.o_kn + h * NOPE : plan.o_kn + (h + 1) * NOPE] = kn_all[h]
        pays[k][:, plan.o_q + plan.heads * NOPE : plan.o_kn] = qr_cat
        pays[k][:, plan.o_kr :] = kr
    for m in range(plan.micro):
        start = pl.multiple_of(m * plan.length + t * plan.share, plan.share)
        x_own[m * plan.share : (m + 1) * plan.share, :] = x[pl.ds(start, plan.share), :]


def key_parts(plan, pay, h):
    qn = pay[:, plan.o_q + h * NOPE : plan.o_q + (h + 1) * NOPE]
    kn = pay[:, plan.o_kn + h * NOPE : plan.o_kn + (h + 1) * NOPE]
    qr = pay[:, plan.o_q + plan.heads * NOPE : plan.o_kn][:, h * ROPE : (h + 1) * ROPE]
    return qn, kn, qr, pay[:, plan.o_kr :]


def query_cotangent(ds, kn, kr, cos, sin):
    return [mm(ds, kn).astype(BF16), rotate_back(mm(ds, kr), cos, sin).astype(BF16)]


def backward_body(plan, last, ranks, top, pieces, pay, v_ref, p_ref, chat_ref, rc_ref, cgain_ref,
                  wq, lat_own, lat_other, wexp, wout, cosine, sine, outs):
    chunks, up_own, tails, dlg_ref, up_s, u_s, d_s, dn_s, dl_s, uc_s = outs
    n, nt = plan.n, plan.nt
    j, t, is_top = ranks[0], ranks[1], ranks[2]
    core = lax.rem(t, 2)
    half = plan.wcol // 2
    if pieces:
        @pl.when(is_top == 1)
        def _():
            up_s[...] = top[...]

        @pl.when(is_top == 0)
        def _():
            for k in range(nt):
                src = lax.rem(t - k + nt, nt)
                for m in range(plan.micro):
                    start = pl.multiple_of(m * plan.length + src * plan.share, plan.share)
                    up_s[pl.ds(start, plan.share), :] = pieces[k][m * plan.share : (m + 1) * plan.share, :]
        up_ref = up_s
    else:
        up_ref = top
    for m in range(plan.micro):
        start = pl.multiple_of(m * plan.length + t * plan.share, plan.share)
        up_own[m * plan.share : (m + 1) * plan.share, :] = up_ref[pl.ds(start, plan.share), :]
    for b in range(n):
        u_s[b] = up_ref[:, b * plan.wcol : (b + 1) * plan.wcol]
    dmixed = jnp.zeros((plan.rows, plan.hcol), F32)
    for k in range(n):
        src = lax.rem(j - k + n, n)
        dmixed = dmixed + mm_nt(u_s[src], wout[k][...])
    dmixed = dmixed.astype(BF16)
    cos, sin = cosine[...], sine[...]
    dq, dexp, dvs, dss = [], [], [], []
    dkr = jnp.zeros((plan.rows, ROPE), F32)
    scale = (NOPE + ROPE) ** (-0.5)
    for h in range(plan.heads):
        qn, kn, qr, kr = key_parts(plan, pay, h)
        v = v_ref[:, h * VDIM : (h + 1) * VDIM]
        p = p_ref[h]
        dm = dmixed[:, h * VDIM : (h + 1) * VDIM]
        dp = mm_nt(dm, v)
        ds = (p * (dp - jnp.sum(dp * p, axis=1, keepdims=True)) * scale).astype(BF16)
        dv = mm_tn(p.astype(BF16), dm).astype(BF16)
        dq.extend(query_cotangent(ds, kn, kr, cos, sin))
        dkr = dkr + mm_tn(ds, qr)
        dexp.extend([mm_tn(ds, qn).astype(BF16), dv])
        dvs.append(dv)
        dss.append(ds)
    dq = jnp.concatenate(dq, axis=1)
    dexp = jnp.concatenate(dexp, axis=1)
    for k in range(n):
        src = lax.rem(j - k + n, n)
        d_s[src] = mm_nt(dexp, wexp[k][...])
    dcomp = jnp.concatenate([d_s[b] for b in range(n)], axis=1)
    chat = chat_ref[...]
    if last:
        dlg_ref[...] = jnp.sum(dcomp * chat, axis=0, keepdims=True)
    dchat = dcomp * cgain_ref[...]
    dlow = rc_ref[...] * (dchat - chat * jnp.mean(dchat * chat, axis=1, keepdims=True))
    dlatent = jnp.concatenate([dlow, rotate_back(dkr, cos, sin)], axis=1).astype(BF16)
    own_at = pl.multiple_of(core * half, half)
    other_at = pl.multiple_of((1 - core) * half, half)
    for k in range(n):
        src = lax.rem(j - k + n, n)
        dn_s[2 * src + core] = (
            mm_nt(dq, wq[k][pl.ds(own_at, half), :]) + mm_nt(dlatent, lat_own[k][...])
        ).astype(BF16)
        dn_s[2 * src + 1 - core] = (
            mm_nt(dq, wq[k][pl.ds(other_at, half), :]) + mm_nt(dlatent, lat_other[k][...])
        ).astype(BF16)
    dl_s[...] = dlatent
    for k in range(nt):
        dst = lax.rem(t + k, nt)
        for m in range(plan.micro):
            start = pl.multiple_of(m * plan.length + dst * plan.share, plan.share)
            at = slice(m * plan.share, (m + 1) * plan.share)
            for b in range(2 * n):
                chunks[k][at, b * half : (b + 1) * half] = dn_s[b, pl.ds(start, plan.share), :]
            if last:
                chunks[k][at, plan.width :] = dl_s[pl.ds(start, plan.share), :]
    if last:
        small = []
        for ds in dss:
            rows = [
                ds[m * plan.length : (m + 1) * plan.length, m * plan.length : (m + 1) * plan.length]
                for m in range(plan.micro)
            ]
            small.append(jnp.concatenate(rows, axis=0))
        ds_cat = jnp.concatenate(small, axis=1)
        for k in range(n):
            dst = lax.rem(j + k, n)
            tails[k][:, : plan.o_dv] = ds_cat
            for h in range(plan.heads):
                tails[k][:, plan.o_dv + h * VDIM : plan.o_dv + (h + 1) * VDIM] = dvs[h]
            tails[k][:, plan.o_up :] = u_s[dst]


def norm_body(plan, last, pieces, up_own, x_own, gain_ref, dlg_ref, dx_ref, dl_ref):
    total = pieces[0][...].astype(F32)
    for piece in pieces[1:]:
        total = total + piece[...].astype(F32)
    dn = total[:, : plan.width]
    x = x_own[...].astype(F32)
    scale = lax.rsqrt(jnp.mean(x * x, axis=1, keepdims=True) + EPS)
    xhat = x * scale
    dhat = dn * gain_ref[...]
    dx = scale * (dhat - xhat * jnp.mean(dhat * xhat, axis=1, keepdims=True))
    dx_ref[...] = (up_own[...].astype(F32) + dx).astype(BF16)
    if last:
        own = plan.micro * plan.share
        dl_ref[...] = jnp.zeros(dl_ref.shape, BF16)
        dl_ref[:own, :] = total[:, plan.width :].astype(BF16)
        dgain = jnp.sum(dn * xhat, axis=0, keepdims=True)
        parts = [dgain[:, i * plan.rank : (i + 1) * plan.rank] for i in range(plan.misc - 1)]
        parts = jnp.concatenate(parts + [dlg_ref[...]], axis=0)
        high = parts.astype(BF16)
        low = (parts - high.astype(F32)).astype(BF16)
        dl_ref[own : own + plan.misc, : plan.rank] = high
        dl_ref[own + plan.misc : own + 2 * plan.misc, : plan.rank] = low


def gradient_body(plan, ranks, pays, tails, dls, cosine, sine, outs):
    g_gain, g_q, g_lat, g_lg, g_exp, g_out, a_n, a_c, a_m, a_u, a_dq, a_de, a_dl, m_s, l_s = outs
    n, nt = plan.n, plan.nt
    j, t = ranks[0], ranks[1]
    cos, sin = cosine[...], sine[...]
    own = plan.micro * plan.share
    misc = jnp.zeros((plan.misc, plan.rank), F32)
    for k in range(n):
        at = slice(k * plan.rows, (k + 1) * plan.rows)
        pay, tail = pays[k], tails[k]
        a_n[at, :] = pay[:, : plan.wcol]
        a_c[at, :] = pay[:, plan.o_comp : plan.o_mixed]
        a_m[at, :] = pay[:, plan.o_mixed : plan.o_q]
        a_u[at, :] = tail[:, plan.o_up :]
        for h in range(plan.heads):
            qn, kn, qr, kr = key_parts(plan, pay, h)
            for m in range(plan.micro):
                part = slice(m * plan.length, (m + 1) * plan.length)
                rows = slice(k * plan.rows + m * plan.length, k * plan.rows + (m + 1) * plan.length)
                ds = tail[part, : plan.o_dv][:, h * plan.length : (h + 1) * plan.length]
                dqn, dqr = query_cotangent(ds, kn[part], kr[part], cos[part], sin[part])
                q_at = h * (NOPE + ROPE)
                a_dq[rows, q_at : q_at + NOPE] = dqn
                a_dq[rows, q_at + NOPE : q_at + NOPE + ROPE] = dqr
                e_at = h * (NOPE + VDIM)
                a_de[rows, e_at : e_at + NOPE] = mm_tn(ds, qn[part]).astype(BF16)
                a_de[rows, e_at + NOPE : e_at + NOPE + VDIM] = tail[part, plan.o_dv + h * VDIM : plan.o_dv + (h + 1) * VDIM]
        for i in range(nt):
            src = lax.rem(t - i + nt, nt)
            base = k * plan.dl_rows
            for m in range(plan.micro):
                start = pl.multiple_of(k * plan.rows + m * plan.length + src * plan.share, plan.share)
                a_dl[pl.ds(start, plan.share), :] = dls[i][base + m * plan.share : base + (m + 1) * plan.share, :]
            rest = dls[i][base + own : base + plan.dl_rows, : plan.rank].astype(F32)
            misc = misc + rest[: plan.misc] + rest[plan.misc : 2 * plan.misc]
    per = plan.rank // plan.wcol
    for b in range(n):
        m_s[b] = misc[b // per : b // per + 1, (b % per) * plan.wcol : (b % per + 1) * plan.wcol]
        l_s[b] = misc[plan.misc - 1 :, b * plan.ccol : (b + 1) * plan.ccol]
    g_gain[...] = m_s[j]
    g_lg[...] = l_s[j]
    g_q[...] = mm_tn(a_n[...], a_dq[...])
    g_exp[...] = mm_tn(a_c[...], a_de[...])
    g_out[...] = mm_tn(a_m[...], a_u[...])
    g_lat[...] = mm_tn(a_n[...], a_dl[...])


def grouped(body, counts_in, n_out_groups, refs):
    out, at = [], 0
    for count in counts_in:
        if count is None:
            out.append(refs[at])
            at += 1
        else:
            out.append(list(refs[at : at + count]))
            at += count
    return out


def kernel_call(body, groups, out_groups, scratch, flops):
    def flat(items):
        return [leaf for item in items for leaf in (item if isinstance(item, list) else [item])]

    counts = [len(g) if isinstance(g, list) else None for g in groups + out_groups] + [None] * len(scratch)

    def kernel(*refs):
        body(*grouped(body, counts, None, refs))

    outs = flat(out_groups)
    vmem = pl.BlockSpec(memory_space=pltpu.VMEM)
    ins = flat(groups)
    got = pl.pallas_call(
        kernel,
        in_specs=[pl.BlockSpec(memory_space=pltpu.SMEM)] + [vmem] * (len(ins) - 1),
        out_specs=[vmem] * len(outs),
        out_shape=outs,
        scratch_shapes=scratch,
        cost_estimate=pl.CostEstimate(flops=flops, bytes_accessed=4 << 20, transcendentals=0),
    )(*ins)
    result, at = [], 0
    for g in out_groups:
        if isinstance(g, list):
            result.append(list(got[at : at + len(g)]))
            at += len(g)
        else:
            result.append(got[at])
            at += 1
    return result


def around(value, axis, count):
    moved = [value]
    for k in range(1, count):
        moved.append(lax.ppermute(value, axis, [(i, (i + k) % count) for i in range(count)]))
    return moved


def handed(values, axis, count):
    moved = [values[0]]
    for k in range(1, count):
        moved.append(lax.ppermute(values[k], axis, [(i, (i + k) % count) for i in range(count)]))
    return moved


def token_shards(plan, saved, top_grad, gain, w_query, w_latent, compressed_gain, expand_weight, w_output):
    n, nt, rows = plan.n, plan.nt, plan.rows
    j = lax.axis_index("dp")
    t = lax.axis_index("tensor")
    section = lax.axis_index("pipe")
    is_top = (section == plan.n_pipe - 1).astype(jnp.int32)
    ranks = jnp.stack([j, t, is_top]).astype(jnp.int32)
    half = plan.wcol // 2
    half_rows = lax.dynamic_slice_in_dim(w_latent[0], lax.rem(t, 2) * half, half, 0)
    gains = around(jnp.concatenate([gain, compressed_gain], axis=1), "dp", n)
    wq = around(w_query[0], "dp", n)
    lat_own = around(half_rows, "dp", n)
    swap = [(i, i ^ 1) for i in range(nt)]
    lat_other = [lax.ppermute(block, "tensor", swap) for block in lat_own]
    wexp = around(expand_weight[0], "dp", n)
    wout = around(w_output[0], "dp", n)
    x = saved[0].reshape(rows, plan.width)
    top = top_grad.reshape(rows, plan.width)
    freq = 10000.0 ** (-np.arange(ROPE // 2) / (ROPE // 2))
    angle = np.tile(np.arange(plan.length)[:, None] * freq[None, :], (plan.micro, 1))
    cosine = jnp.asarray(np.concatenate([np.cos(angle), np.cos(angle)], axis=1), F32)
    sine = jnp.asarray(np.concatenate([-np.sin(angle), np.sin(angle)], axis=1), F32)

    def shape(dims, kind=BF16):
        return jax.ShapeDtypeStruct(dims, kind)

    own = plan.micro * plan.share

    def forward(ranks, x, gains, wq, lo, lt, we, cosine, sine, *outs):
        forward_body(plan, ranks, x, gains, wq, lo, lt, we, cosine, sine, outs)

    pays, v, p, chat, rc, gain32, cgain32, x_own = kernel_call(
        forward,
        [ranks, x, gains, wq, lat_own, lat_other, wexp, cosine, sine],
        [
            [shape((rows, plan.pay))] * n,
            shape((rows, plan.hcol)),
            shape((plan.heads, rows, rows), F32),
            shape((rows, plan.rank), F32),
            shape((rows, 1), F32),
            shape((1, plan.width), F32),
            shape((1, plan.rank), F32),
            shape((own, plan.width)),
        ],
        [
            pltpu.VMEM((n, 1, plan.wcol), F32),
            pltpu.VMEM((n, 1, plan.ccol), F32),
            pltpu.VMEM((n, rows, plan.wcol), BF16),
            pltpu.VMEM((2 * n, rows, half), BF16),
            pltpu.VMEM((n, rows, plan.ccol), BF16),
        ],
        5 * 10**8,
    )
    pieces = []
    for tick in range(plan.n_pipe):
        last = tick == plan.n_pipe - 1

        def backward(ranks, top, pieces, pay, v, p, chat, rc, cg, wq, lo, lt, we, wo, cosine, sine, *outs):
            outs = list(outs)
            if not last:
                outs[2:2] = [None, None]
            backward_body(plan, last, ranks, top, pieces, pay, v, p, chat, rc, cg, wq, lo, lt, we, wo, cosine, sine, outs)

        chunk = plan.width + (plan.latent if last else 0)
        out_groups = [[shape((own, chunk))] * nt, shape((own, plan.width))]
        if last:
            out_groups += [[shape((rows, plan.tail))] * n, shape((1, plan.rank), F32)]
        got = kernel_call(
            backward,
            [ranks, top, pieces, pays[0], v, p, chat, rc, cgain32, wq, lat_own, lat_other, wexp, wout, cosine, sine],
            out_groups,
            [
                pltpu.VMEM((rows, plan.width), BF16),
                pltpu.VMEM((n, rows, plan.wcol), BF16),
                pltpu.VMEM((n, rows, plan.ccol), F32),
                pltpu.VMEM((2 * n, rows, half), BF16),
                pltpu.VMEM((rows, plan.latent), BF16),
                pltpu.VMEM((8, 128), BF16),
            ],
            10**9,
        )
        chunks, up_own = got[0], got[1]
        sums = handed(chunks, "tensor", nt)
        norm_in = [ranks, sums, up_own, x_own, gain32]
        norm_out = [shape((own, plan.width))]
        if last:
            tails, dlg = got[2], got[3]
            norm_in.append(dlg)
            norm_out.append(shape((plan.dl_rows, plan.latent)))

        def norm(ranks, sums, up_own, x_own, gain32, *rest):
            dlg, dx, dl = rest if last else (None, rest[0], None)
            norm_body(plan, last, sums, up_own, x_own, gain32, dlg, dx, dl)

        got = kernel_call(norm, norm_in, norm_out, [], 10**6)
        dx = got[0]
        if not last:
            pieces = []
            for k in range(nt):
                pairs = [
                    (s * nt + i, (s - 1) * nt + (i + k) % nt) for s in range(1, plan.n_pipe) for i in range(nt)
                ]
                pieces.append(lax.ppermute(dx, ("pipe", "tensor"), pairs))
    dl = got[1]
    pays = handed(pays, "dp", n)
    tails = handed(tails, "dp", n)
    dls = around(jnp.concatenate(around(dl, "dp", n), axis=0), "tensor", nt)

    def gradients(ranks, pays, tails, dls, cosine, sine, *outs):
        gradient_body(plan, ranks, pays, tails, dls, cosine, sine, outs)

    every = n * rows
    g_gain, g_q, g_lat, g_lg, g_exp, g_out = kernel_call(
        gradients,
        [ranks, pays, tails, dls, cosine, sine],
        [
            shape((1, plan.wcol), F32),
            shape((plan.wcol, plan.qcol), F32),
            shape((plan.wcol, plan.latent), F32),
            shape((1, plan.ccol), F32),
            shape((plan.ccol, plan.heads * (NOPE + VDIM)), F32),
            shape((plan.hcol, plan.wcol), F32),
        ],
        [
            pltpu.VMEM((every, plan.wcol), BF16),
            pltpu.VMEM((every, plan.ccol), BF16),
            pltpu.VMEM((every, plan.hcol), BF16),
            pltpu.VMEM((every, plan.wcol), BF16),
            pltpu.VMEM((every, plan.qcol), BF16),
            pltpu.VMEM((every, plan.heads * (NOPE + VDIM)), BF16),
            pltpu.VMEM((every, plan.latent), BF16),
            pltpu.VMEM((n, 1, plan.wcol), F32),
            pltpu.VMEM((n, 1, plan.ccol), F32),
        ],
        10**9,
    )
    results = dx.reshape(plan.micro, plan.share, plan.width)
    return results[None], g_gain, g_q[None], g_lat[None], g_lg, g_exp[None], g_out[None]


def shards(saved, top_grad, gain, w_query, w_latent, compressed_gain, expand_weight, w_output):
    args = (saved, top_grad, gain, w_query, w_latent, compressed_gain, expand_weight, w_output)
    sizes = [lax.axis_size(axis) for axis in ("pipe", "dp", "tensor")]
    plan = Plan(saved, w_query, w_latent, expand_weight, w_output, *sizes)
    if plan.fits():
        return token_shards(plan, *args)
    return plain_shards(*args)


def solution(mesh):
    in_specs = (
        P("pipe", None, "dp", None),
        P(None, "dp", None),
        P("pipe", "dp"),
        P("pipe", "dp", "tensor"),
        P("pipe", "dp", None),
        P("pipe", "dp"),
        P("pipe", "dp", "tensor"),
        P("pipe", "tensor", "dp"),
    )
    out_specs = (
        P("pipe", None, ("dp", "tensor"), None),
        P("pipe", "dp"),
        P("pipe", "dp", "tensor"),
        P("pipe", "dp", None),
        P("pipe", "dp"),
        P("pipe", "dp", "tensor"),
        P("pipe", "tensor", "dp"),
    )
    return jax.shard_map(shards, mesh=mesh, in_specs=in_specs, out_specs=out_specs, check_vma=False)
```

```python
import functools

import jax
import jax.numpy as jnp
import numpy as np
from jax import lax
from jax.experimental import pallas as pl
from jax.experimental.pallas import tpu as pltpu
from jax.sharding import PartitionSpec as P

NOPE = 128
ROPE = 64
VDIM = 128
COMPRESSED_RANK = 512


EPS = 1e-06


def passed_along(value, axis, steps):
    count = lax.axis_size(axis)
    first, last = (max(0, -steps), min(count, count - steps))
    return lax.ppermute(value, axis, [(source, source + steps) for source in range(first, last)])


def root_mean_scale(values, scale):
    return values * lax.rsqrt(jnp.mean(values * values, axis=-1, keepdims=True) + EPS) * scale


def rotary_angles(values):
    length = values.shape[0]
    half = values.shape[-1] // 2
    freq = jnp.exp(-jnp.log(10000.0) * jnp.arange(half, dtype=jnp.float32) / half)
    angle = jnp.arange(length, dtype=jnp.float32)[:, None] * freq[None, :]
    cosine = jnp.cos(angle)[:, None, :]
    sine = jnp.sin(angle)[:, None, :]
    first = values[..., :half]
    second = values[..., half:]
    return jnp.concatenate(
        [first * cosine - second * sine, second * cosine + first * sine], axis=-1
    )


def branch(normed, w_q, w_lat, latent_norm_gain, w_exp, w_out):
    length = normed.shape[0]
    heads = w_q.shape[1] // (NOPE + ROPE)
    rounded = normed.astype(jnp.bfloat16)
    query = jnp.dot(rounded, w_q, preferred_element_type=jnp.float32).reshape(
        length, heads, NOPE + ROPE
    )
    latent_state = jnp.dot(rounded, w_lat, preferred_element_type=jnp.float32)
    compressed_state = root_mean_scale(latent_state[:, :COMPRESSED_RANK], latent_norm_gain).astype(
        jnp.bfloat16
    )
    rotary_key_part = rotary_angles(latent_state[:, None, COMPRESSED_RANK:])[:, 0, :]
    expanded = jnp.dot(compressed_state, w_exp, preferred_element_type=jnp.float32).reshape(
        length, heads, NOPE + VDIM
    )
    key_nope = expanded[:, :, :NOPE]
    values = expanded[:, :, NOPE:].astype(jnp.bfloat16)
    query_rope = rotary_angles(query[:, :, NOPE:])
    scores = jnp.einsum("qhd,khd->hqk", query[:, :, :NOPE], key_nope) + jnp.einsum(
        "qhd,kd->hqk", query_rope, rotary_key_part
    )
    scores = scores * (NOPE + ROPE) ** (-0.5)
    causal = jnp.arange(length)[:, None] >= jnp.arange(length)[None, :]
    scores = jnp.where(causal[None], scores, -1e30)
    weights = jax.nn.softmax(scores, axis=-1).astype(jnp.bfloat16)
    mixed = jnp.einsum("hqk,khd->qhd", weights.astype(jnp.float32), values.astype(jnp.float32))
    mixed = mixed.astype(jnp.bfloat16).reshape(length, heads * VDIM)
    return jnp.dot(mixed, w_out, preferred_element_type=jnp.float32)


def plain_shards(saved, top_grad, gain, w_query, w_latent, compressed_gain, expand_weight, w_output):
    gathered = (
        lax.all_gather(gain, "dp", axis=1, tiled=True),
        lax.all_gather(w_query, "dp", axis=1, tiled=True),
        lax.all_gather(w_latent, "dp", axis=1, tiled=True),
        lax.all_gather(compressed_gain, "dp", axis=1, tiled=True),
        lax.all_gather(expand_weight, "dp", axis=1, tiled=True),
        lax.all_gather(w_output, "dp", axis=2, tiled=True),
    )
    gain32 = gathered[0][0].astype(jnp.float32)
    query_all = gathered[1][0]
    latent_all = gathered[2][0]
    lgain32 = gathered[3][0].astype(jnp.float32)
    expand_all = gathered[4][0]
    output_all = gathered[5][0]
    sections = lax.axis_size("pipe")
    section_index = lax.axis_index("pipe")
    tensor_count = lax.axis_size("tensor")
    tensor_rank = lax.axis_index("tensor")
    micro_count = saved.shape[1]
    length = saved.shape[2]
    width = saved.shape[3]
    share = length // tensor_count

    def compute(normed, upstream):
        unused, pull = jax.vjp(
            lambda value: branch(value, query_all, latent_all, lgain32, expand_all, output_all),
            normed,
        )
        return pull(upstream.astype(jnp.float32))[0]

    def skip(normed, upstream):
        return jnp.zeros_like(normed)

    gain_total = jnp.zeros((width,), jnp.float32)
    results = jnp.zeros((micro_count, share, width), jnp.bfloat16)
    stored = jnp.zeros((micro_count, length, width), jnp.bfloat16)
    received = jnp.zeros((length, width), jnp.bfloat16)
    for tick in range(sections + micro_count - 1):
        micro = tick - (sections - 1 - section_index)
        active = jnp.logical_and(micro >= 0, micro < micro_count)
        picked = jnp.clip(micro, 0, micro_count - 1)
        x_rows = lax.dynamic_index_in_dim(saved[0], picked, 0, keepdims=False)
        top_rows = lax.dynamic_index_in_dim(top_grad, picked, 0, keepdims=False)
        arrived = received
        upstream = jnp.where(section_index == sections - 1, top_rows, arrived)
        x_float = x_rows.astype(jnp.float32)
        normed, norm_pull = jax.vjp(root_mean_scale, x_float, gain32)
        branch_grad = lax.cond(active, compute, skip, normed, upstream)
        d_normed = lax.psum(branch_grad.astype(jnp.bfloat16), "tensor").astype(jnp.float32)
        dx_norm, d_gain = norm_pull(d_normed)
        dx = (upstream.astype(jnp.float32) + dx_norm).astype(jnp.bfloat16)
        gain_total = gain_total + jnp.where(active, d_gain, 0.0)
        mine = lax.dynamic_slice_in_dim(dx, tensor_rank * share, share, 0)
        chosen = (jnp.arange(micro_count) == micro)[:, None, None]
        results = jnp.where(chosen, mine[None], results)
        stored = jnp.where(chosen, upstream[None], stored)
        received = passed_along(dx, "pipe", -1)
    totals = (
        jnp.zeros(query_all.shape, jnp.float32),
        jnp.zeros(latent_all.shape, jnp.float32),
        jnp.zeros(lgain32.shape, jnp.float32),
        jnp.zeros(expand_all.shape, jnp.float32),
        jnp.zeros(output_all.shape, jnp.float32),
    )
    for micro_index in range(micro_count):
        normed_again = root_mean_scale(saved[0, micro_index].astype(jnp.float32), gain32)
        unused, weight_pull = jax.vjp(
            lambda w_q, w_lat, lat_gain, w_exp, w_out: branch(
                normed_again, w_q, w_lat, lat_gain, w_exp, w_out
            ),
            query_all,
            latent_all,
            lgain32,
            expand_all,
            output_all,
        )
        cotangents = weight_pull(stored[micro_index].astype(jnp.float32))
        totals = tuple(
            (total + piece.astype(jnp.float32) for total, piece in zip(totals, cotangents))
        )
    gain_part = jnp.where(tensor_rank == 0, gain_total, 0.0)
    grad_q, grad_lat, grad_lg, grad_e, grad_o = totals
    out_q, part_lat, part_lg, out_e, out_o, part_gain = (
        lax.psum_scatter(grad_q.astype(jnp.bfloat16), "dp", scatter_dimension=0, tiled=True).astype(
            jnp.float32
        ),
        lax.psum_scatter(
            grad_lat.astype(jnp.bfloat16), "dp", scatter_dimension=0, tiled=True
        ).astype(jnp.float32),
        lax.psum_scatter(
            grad_lg.astype(jnp.bfloat16), "dp", scatter_dimension=0, tiled=True
        ).astype(jnp.float32),
        lax.psum_scatter(grad_e.astype(jnp.bfloat16), "dp", scatter_dimension=0, tiled=True).astype(
            jnp.float32
        ),
        lax.psum_scatter(grad_o.astype(jnp.bfloat16), "dp", scatter_dimension=1, tiled=True).astype(
            jnp.float32
        ),
        lax.psum_scatter(
            gain_part.astype(jnp.bfloat16), "dp", scatter_dimension=0, tiled=True
        ).astype(jnp.float32),
    )
    out_lat, out_lg, out_gain = (
        lax.psum(part_lat.astype(jnp.bfloat16), "tensor").astype(jnp.float32),
        lax.psum(part_lg.astype(jnp.bfloat16), "tensor").astype(jnp.float32),
        lax.psum(part_gain.astype(jnp.bfloat16), "tensor").astype(jnp.float32),
    )
    return (
        results[None],
        out_gain[None],
        out_q[None],
        out_lat[None],
        out_lg[None],
        out_e[None],
        out_o[None],
    )


F32 = jnp.float32
BF16 = jnp.bfloat16


def mm(a, b):
    return lax.dot_general(a, b, (((1,), (0,)), ((), ())), preferred_element_type=F32)


def mm_nt(a, b):
    return lax.dot_general(a, b, (((1,), (1,)), ((), ())), preferred_element_type=F32)


def mm_tn(a, b):
    return lax.dot_general(a, b, (((0,), (0,)), ((), ())), preferred_element_type=F32)


def turned(values):
    half = values.shape[1] // 2
    return jnp.concatenate([values[:, half:], values[:, :half]], axis=1)


def rotate(values, cosine, sine):
    return values * cosine + turned(values) * sine


def rotate_back(values, cosine, sine):
    return values * cosine - turned(values) * sine


class Plan:
    def __init__(self, saved, w_query, w_latent, expand_weight, w_output, n_pipe, n_dp, n_tensor):
        self.n_pipe, self.n, self.nt = n_pipe, n_dp, n_tensor
        self.micro, self.length, self.width = saved.shape[1:]
        self.rows = self.micro * self.length
        self.share = self.length // n_tensor
        self.heads = w_query.shape[2] // (NOPE + ROPE)
        self.rank = expand_weight.shape[1] * n_dp
        self.latent = w_latent.shape[2]
        self.wcol = self.width // n_dp
        self.ccol = self.rank // n_dp
        self.qcol = self.heads * (NOPE + ROPE)
        self.hcol = self.heads * VDIM
        self.rope_all = self.heads * ROPE
        self.o_mixed = 0
        self.o_q = self.o_mixed + self.hcol
        self.o_kn = self.o_q + self.qcol
        self.o_kr = self.o_kn + self.heads * NOPE
        self.pay = self.o_kr + ROPE
        self.o_dv = self.heads * self.length
        self.o_up = self.o_dv + self.hcol
        self.tail = self.o_up
        self.own = self.micro * self.share
        self.half = self.rows // 2
        self.spare = -self.latent % 128
        self.lrow = self.rank // max(self.spare, 1)
        self.grow = self.width // max(self.spare, 1)
        self.chunk = self.width + self.latent + self.spare

    def fits(self):
        aligned = self.wcol % 256 == 0 and self.ccol % 128 == 0 and self.rope_all % 128 == 0
        whole = (self.heads * self.length) % 128 == 0 and self.latent % 32 == 0
        if self.spare == 0 or self.rank % self.spare or self.wcol % self.spare:
            return False
        room = 2 * (self.lrow + self.grow) <= self.half
        few = self.n & (self.n - 1) == 0 and self.rows <= 512
        return aligned and whole and room and few and self.nt % 2 == 0 and self.share % 16 == 0


def share_rows(plan, core):
    at = 0
    for chip in range(plan.nt // 2):
        for m in range(plan.micro):
            start = m * plan.length + (2 * chip + core) * plan.share
            yield pl.multiple_of(start, plan.share), slice(at, at + plan.share)
            at += plan.share


def assemble_latent(plan, core, lat_own, lat_other, w_s):
    part = plan.latent // 2
    for k in range(plan.n):
        w_s[k, pl.ds(pl.multiple_of(core * part, 16), part), :] = lat_own[k][...]
        w_s[k, pl.ds(pl.multiple_of((1 - core) * part, 16), part), :] = lat_other[k][...]


def forward_body(plan, ranks, x, gains, wq, lat_own, lat_other, wexp, cosine, sine, outs):
    (sent, pay, v_ref, p_ref, chat_ref, rc_ref, gain_ref, cgain_ref, x_own, wlat, g_s, cg_s, n_s, c_s) = outs
    n = plan.n
    j, t = ranks[0], ranks[1]
    core = lax.rem(t, 2)
    assemble_latent(plan, core, lat_own, lat_other, wlat)
    for k in range(n):
        src = j ^ k
        g_s[src] = gains[k][:, : plan.wcol].astype(F32)
        cg_s[src] = gains[k][:, plan.wcol :].astype(F32)
    xf = x[...].astype(F32)
    scale = lax.rsqrt(jnp.mean(xf * xf, axis=1, keepdims=True) + EPS)
    for b in range(n):
        block = xf[:, b * plan.wcol : (b + 1) * plan.wcol] * scale * g_s[b]
        rounded = block.astype(BF16)
        n_s[b] = rounded
        gain_ref[:, b * plan.wcol : (b + 1) * plan.wcol] = g_s[b]
        cgain_ref[:, b * plan.ccol : (b + 1) * plan.ccol] = cg_s[b]
    query = jnp.zeros((plan.rows, plan.qcol), F32)
    latent = jnp.zeros((plan.rows, plan.latent), F32)
    for k in range(n):
        query = query + mm(n_s[j ^ k], wq[k][...])
        latent = latent + mm_nt(n_s[j ^ k], wlat[k])
    low = latent[:, : plan.rank]
    rc = lax.rsqrt(jnp.mean(low * low, axis=1, keepdims=True) + EPS)
    chat = low * rc
    chat_ref[...] = chat
    rc_ref[...] = rc
    comp = (chat * cgain_ref[...]).astype(BF16)
    for b in range(n):
        c_s[b] = comp[:, b * plan.ccol : (b + 1) * plan.ccol]
    expanded = jnp.zeros((plan.rows, plan.heads * (NOPE + VDIM)), F32)
    for k in range(n):
        expanded = expanded + mm(c_s[j ^ k], wexp[k][...])
    cos, sin = cosine[...], sine[...]
    kr = rotate(latent[:, plan.rank :], cos, sin).astype(BF16)
    row = lax.broadcasted_iota(jnp.int32, (plan.rows, plan.rows), 0)
    col = lax.broadcasted_iota(jnp.int32, (plan.rows, plan.rows), 1)
    keep = row >= col
    for m in range(1, plan.micro):
        keep = keep & ((row < m * plan.length) | (col >= m * plan.length))
    qn_all, qr_all, kn_all, mixed_all = [], [], [], []
    for h in range(plan.heads):
        q_at = h * (NOPE + ROPE)
        e_at = h * (NOPE + VDIM)
        qn = query[:, q_at : q_at + NOPE].astype(BF16)
        qr = rotate(query[:, q_at + NOPE : q_at + NOPE + ROPE], cos, sin).astype(BF16)
        kn = expanded[:, e_at : e_at + NOPE].astype(BF16)
        v = expanded[:, e_at + NOPE : e_at + NOPE + VDIM].astype(BF16)
        scores = (mm_nt(qn, kn) + mm_nt(qr, kr)) * (NOPE + ROPE) ** (-0.5)
        scores = jnp.where(keep, scores, -1e30)
        top = jnp.max(scores, axis=1, keepdims=True)
        e = jnp.exp(scores - top)
        p = e / jnp.sum(e, axis=1, keepdims=True)
        p_ref[h] = p
        mixed = mm(p.astype(BF16), v).astype(BF16)
        v_ref[:, h * VDIM : (h + 1) * VDIM] = v
        qn_all.append(qn)
        qr_all.append(qr)
        kn_all.append(kn)
        mixed_all.append(mixed)
    qr_cat = jnp.concatenate(qr_all, axis=1)
    for k in range(n):
        sent[k][:, : plan.wcol] = n_s[j ^ k]
        sent[k][:, plan.wcol :] = c_s[j ^ k]
    for h in range(plan.heads):
        pay[:, plan.o_mixed + h * VDIM : plan.o_mixed + (h + 1) * VDIM] = mixed_all[h]
        pay[:, plan.o_q + h * NOPE : plan.o_q + (h + 1) * NOPE] = qn_all[h]
        pay[:, plan.o_kn + h * NOPE : plan.o_kn + (h + 1) * NOPE] = kn_all[h]
    pay[:, plan.o_q + plan.heads * NOPE : plan.o_kn] = qr_cat
    pay[:, plan.o_kr :] = kr
    for start, at in share_rows(plan, core):
        x_own[at, :] = x[pl.ds(start, plan.share), :]


def key_parts(plan, pay, h):
    qn = pay[:, plan.o_q + h * NOPE : plan.o_q + (h + 1) * NOPE]
    kn = pay[:, plan.o_kn + h * NOPE : plan.o_kn + (h + 1) * NOPE]
    qr = pay[:, plan.o_q + plan.heads * NOPE : plan.o_kn][:, h * ROPE : (h + 1) * ROPE]
    return qn, kn, qr, pay[:, plan.o_kr :]


def query_cotangent(ds, kn, kr, cos, sin):
    return [mm(ds, kn).astype(BF16), rotate_back(mm(ds, kr), cos, sin).astype(BF16)]


def backward_body(plan, last, ranks, top, pieces, pay, v_ref, p_ref, chat_ref, rc_ref, cgain_ref,
                  wq, wlat, wexp, wout, cosine, sine, outs):
    chunks, up_own, tail, ups, up_s, u_s, d_s, dn_s, dl_s = outs
    n = plan.n
    j, t, is_top = ranks[0], ranks[1], ranks[2]
    core = lax.rem(t, 2)
    if pieces:
        @pl.when(is_top == 1)
        def _():
            up_s[...] = top[...]

        @pl.when(is_top == 0)
        def _():
            for piece, side in zip(pieces, (core, 1 - core)):
                for start, at in share_rows(plan, side):
                    up_s[pl.ds(start, plan.share), :] = piece[at, :]

        up_ref = up_s
    else:
        up_ref = top
    for start, at in share_rows(plan, core):
        up_own[at, :] = up_ref[pl.ds(start, plan.share), :]
    for b in range(n):
        u_s[b] = up_ref[:, b * plan.wcol : (b + 1) * plan.wcol]
    dmixed = jnp.zeros((plan.rows, plan.hcol), F32)
    for k in range(n):
        dmixed = dmixed + mm_nt(u_s[j ^ k], wout[k][...])
    dmixed = dmixed.astype(BF16)
    cos, sin = cosine[...], sine[...]
    dq, dexp, dvs, dss = [], [], [], []
    dkr = jnp.zeros((plan.rows, ROPE), F32)
    scale = (NOPE + ROPE) ** (-0.5)
    for h in range(plan.heads):
        qn, kn, qr, kr = key_parts(plan, pay, h)
        v = v_ref[:, h * VDIM : (h + 1) * VDIM]
        p = p_ref[h]
        dm = dmixed[:, h * VDIM : (h + 1) * VDIM]
        dp = mm_nt(dm, v)
        ds = (p * (dp - jnp.sum(dp * p, axis=1, keepdims=True)) * scale).astype(BF16)
        dv = mm_tn(p.astype(BF16), dm).astype(BF16)
        dq.extend(query_cotangent(ds, kn, kr, cos, sin))
        dkr = dkr + mm_tn(ds, qr)
        dexp.extend([mm_tn(ds, qn).astype(BF16), dv])
        dvs.append(dv)
        dss.append(ds)
    dq = jnp.concatenate(dq, axis=1)
    dexp = jnp.concatenate(dexp, axis=1)
    for k in range(n):
        d_s[j ^ k] = mm_nt(dexp, wexp[k][...])
    dcomp = jnp.concatenate([d_s[b] for b in range(n)], axis=1)
    chat = chat_ref[...]
    dchat = dcomp * cgain_ref[...]
    dlow = rc_ref[...] * (dchat - chat * jnp.mean(dchat * chat, axis=1, keepdims=True))
    dlatent = jnp.concatenate([dlow, rotate_back(dkr, cos, sin)], axis=1).astype(BF16)
    for k in range(n):
        dn_s[j ^ k] = (mm_nt(dq, wq[k][...]) + mm(dlatent, wlat[k])).astype(BF16)
    if last:
        dl_s[:, : plan.latent] = dlatent
        dl_s[:, plan.latent :] = jnp.zeros((plan.rows, plan.spare), BF16)
    for chunk, side in zip(chunks, (core, 1 - core)):
        for start, at in share_rows(plan, side):
            for b in range(n):
                chunk[at, b * plan.wcol : (b + 1) * plan.wcol] = dn_s[b, pl.ds(start, plan.share), :]
            if last:
                chunk[at, plan.width :] = dl_s[pl.ds(start, plan.share), :]
        if last:
            put_split(plan, chunk, plan.width + plan.latent, 0, jnp.sum(dcomp * chat, axis=0, keepdims=True))
    if last:
        small = []
        for ds in dss:
            rows = [
                ds[m * plan.length : (m + 1) * plan.length, m * plan.length : (m + 1) * plan.length]
                for m in range(plan.micro)
            ]
            small.append(jnp.concatenate(rows, axis=0))
        ds_cat = jnp.concatenate(small, axis=1)
        tail[:, : plan.o_dv] = ds_cat
        for h in range(plan.heads):
            tail[:, plan.o_dv + h * VDIM : plan.o_dv + (h + 1) * VDIM] = dvs[h]
        for k in range(n):
            ups[k][...] = u_s[j ^ k]


def put_split(plan, ref, col, row, values):
    count = values.shape[1] // plan.spare
    high = values.astype(BF16)
    low = (values - high.astype(F32)).astype(BF16)
    for i in range(count):
        piece = slice(i * plan.spare, (i + 1) * plan.spare)
        ref[row + i : row + i + 1, col : col + plan.spare] = high[:, piece]
        ref[row + count + i : row + count + i + 1, col : col + plan.spare] = low[:, piece]


def norm_body(plan, last, ranks, pieces, up_own, x_own, gain_ref, dx_ref, dl_ref, dx_s):
    total = pieces[0][...].astype(F32)
    for piece in pieces[1:]:
        total = total + piece[...].astype(F32)
    dn = total[:, : plan.width]
    x = x_own[...].astype(F32)
    scale = lax.rsqrt(jnp.mean(x * x, axis=1, keepdims=True) + EPS)
    xhat = x * scale
    dhat = dn * gain_ref[...]
    dx = scale * (dhat - xhat * jnp.mean(dhat * xhat, axis=1, keepdims=True))
    dx = (up_own[...].astype(F32) + dx).astype(BF16)
    if not last:
        dx_ref[...] = dx
        return
    dx_s[...] = dx
    at = pl.multiple_of(lax.div(ranks[1], 2) * plan.own, plan.own)
    dx_ref[...] = dx_s[pl.ds(at, plan.own), :]
    rest = total[:, plan.width :]
    dl_ref[...] = rest.astype(BF16)
    lgain = rest[: plan.lrow, plan.latent :] + rest[plan.lrow : 2 * plan.lrow, plan.latent :]
    high = lgain.astype(BF16)
    dl_ref[: plan.lrow, plan.latent :] = high
    dl_ref[plan.lrow : 2 * plan.lrow, plan.latent :] = (lgain - high.astype(F32)).astype(BF16)
    put_split(plan, dl_ref, plan.latent, 2 * plan.lrow, jnp.sum(dn * xhat, axis=0, keepdims=True))


def gradient_body(plan, ranks, sent, pays, tails, ups, dl_own, dl_other, cosine, sine, outs):
    g_gain, g_q, g_lat, g_lg, g_exp, g_out, a_n, a_c, a_m, a_u, a_dq, a_de, a_dl, m_s, l_s = outs
    n = plan.n
    j, t = ranks[0], ranks[1]
    core = lax.rem(t, 2)
    cos, sin = cosine[...], sine[...]
    lgain = jnp.zeros((plan.lrow, plan.spare), F32)
    ggain = jnp.zeros((plan.grow, plan.spare), F32)
    for k in range(n):
        at = slice(k * plan.rows, (k + 1) * plan.rows)
        pay, tail = pays[k], tails[k]
        a_n[at, :] = sent[k][:, : plan.wcol]
        a_c[at, :] = sent[k][:, plan.wcol :]
        a_m[at, :] = pay[:, plan.o_mixed : plan.o_q]
        a_u[at, :] = ups[k][...]
        for h in range(plan.heads):
            qn, kn, qr, kr = key_parts(plan, pay, h)
            for m in range(plan.micro):
                part = slice(m * plan.length, (m + 1) * plan.length)
                rows = slice(k * plan.rows + m * plan.length, k * plan.rows + (m + 1) * plan.length)
                ds = tail[part, : plan.o_dv][:, h * plan.length : (h + 1) * plan.length]
                dqn, dqr = query_cotangent(ds, kn[part], kr[part], cos[part], sin[part])
                q_at = h * (NOPE + ROPE)
                a_dq[rows, q_at : q_at + NOPE] = dqn
                a_dq[rows, q_at + NOPE : q_at + NOPE + ROPE] = dqr
                e_at = h * (NOPE + VDIM)
                a_de[rows, e_at : e_at + NOPE] = mm_tn(ds, qn[part]).astype(BF16)
                a_de[rows, e_at + NOPE : e_at + NOPE + VDIM] = tail[part, plan.o_dv + h * VDIM : plan.o_dv + (h + 1) * VDIM]
        for block, side in ((dl_own[k], core), (dl_other[k], 1 - core)):
            for start, part in share_rows(plan, side):
                a_dl[pl.ds(pl.multiple_of(k * plan.rows + start, plan.share), plan.share), :] = block[part, : plan.latent]
            extra = block[:, plan.latent :].astype(F32)
            if side is core:
                lgain = lgain + extra[: plan.lrow] + extra[plan.lrow : 2 * plan.lrow]
            at_gain = 2 * plan.lrow
            ggain = ggain + extra[at_gain : at_gain + plan.grow] + extra[at_gain + plan.grow : at_gain + 2 * plan.grow]
    wide, low = plan.wcol // plan.spare, plan.ccol // plan.spare
    for b in range(n):
        for i in range(wide):
            m_s[b, :, i * plan.spare : (i + 1) * plan.spare] = ggain[b * wide + i : b * wide + i + 1, :]
        for i in range(low):
            l_s[b, :, i * plan.spare : (i + 1) * plan.spare] = lgain[b * low + i : b * low + i + 1, :]
    g_gain[...] = m_s[j]
    g_lg[...] = l_s[j]
    g_q[...] = mm_tn(a_n[...], a_dq[...])
    g_exp[...] = mm_tn(a_c[...], a_de[...])
    g_out[...] = mm_tn(a_m[...], a_u[...])
    g_lat[...] = mm_tn(a_dl[...], a_n[...])


def grouped(body, counts_in, n_out_groups, refs):
    out, at = [], 0
    for count in counts_in:
        if count is None:
            out.append(refs[at])
            at += 1
        else:
            out.append(list(refs[at : at + count]))
            at += count
    return out


def kernel_call(body, groups, out_groups, scratch, flops):
    def flat(items):
        return [leaf for item in items for leaf in (item if isinstance(item, list) else [item])]

    counts = [len(g) if isinstance(g, list) else None for g in groups + out_groups] + [None] * len(scratch)

    def kernel(*refs):
        body(*grouped(body, counts, None, refs))

    outs = flat(out_groups)
    vmem = pl.BlockSpec(memory_space=pltpu.VMEM)
    ins = flat(groups)
    got = pl.pallas_call(
        kernel,
        in_specs=[pl.BlockSpec(memory_space=pltpu.SMEM)] + [vmem] * (len(ins) - 1),
        out_specs=[vmem] * len(outs),
        out_shape=outs,
        scratch_shapes=scratch,
        compiler_params=pltpu.CompilerParams(vmem_limit_bytes=20 << 20),
        cost_estimate=pl.CostEstimate(flops=flops, bytes_accessed=4 << 20, transcendentals=0),
    )(*ins)
    result, at = [], 0
    for g in out_groups:
        if isinstance(g, list):
            result.append(list(got[at : at + len(g)]))
            at += len(g)
        else:
            result.append(got[at])
            at += 1
    return result


def exchange(value, axis, count, bit):
    return lax.ppermute(value, axis, [(i, i ^ bit) for i in range(count)])


def gathered(value, axis, count):
    blocks = {0: value}
    bit = count // 2
    while bit:
        blocks.update({k | bit: exchange(blocks[k], axis, count, bit) for k in sorted(blocks)})
        bit //= 2
    return [blocks[k] for k in range(count)]


def handed(values, axis, count):
    return [values[0]] + [exchange(values[k], axis, count, k) for k in range(1, count)]


def token_shards(plan, saved, top_grad, gain, w_query, w_latent, compressed_gain, expand_weight, w_output):
    n, nt, rows = plan.n, plan.nt, plan.rows
    j = lax.axis_index("dp")
    t = lax.axis_index("tensor")
    section = lax.axis_index("pipe")
    is_top = (section == plan.n_pipe - 1).astype(jnp.int32)
    ranks = jnp.stack([j, t, is_top]).astype(jnp.int32)
    part = plan.latent // 2
    half_rows = lax.dynamic_slice_in_dim(w_latent[0].T, lax.rem(t, 2) * part, part, 0)
    gains = gathered(jnp.concatenate([gain, compressed_gain], axis=1), "dp", n)
    lat_own = gathered(half_rows, "dp", n)
    lat_other = [exchange(block, "tensor", nt, 1) for block in lat_own]
    wq = gathered(w_query[0], "dp", n)
    wexp = gathered(expand_weight[0], "dp", n)
    wout = gathered(w_output[0], "dp", n)
    x = saved[0].reshape(rows, plan.width)
    top = top_grad.reshape(rows, plan.width)
    freq = 10000.0 ** (-np.arange(ROPE // 2) / (ROPE // 2))
    angle = np.tile(np.arange(plan.length)[:, None] * freq[None, :], (plan.micro, 1))
    cosine = jnp.asarray(np.concatenate([np.cos(angle), np.cos(angle)], axis=1), F32)
    sine = jnp.asarray(np.concatenate([-np.sin(angle), np.sin(angle)], axis=1), F32)

    def shape(dims, kind=BF16):
        return jax.ShapeDtypeStruct(dims, kind)

    def forward(ranks, x, gains, wq, lo, lt, we, cosine, sine, *outs):
        forward_body(plan, ranks, x, gains, wq, lo, lt, we, cosine, sine, outs)

    sent, pay, v, p, chat, rc, gain32, cgain32, x_own, wlat = kernel_call(
        forward,
        [ranks, x, gains, wq, lat_own, lat_other, wexp, cosine, sine],
        [
            [shape((rows, plan.wcol + plan.ccol))] * n,
            shape((rows, plan.pay)),
            shape((rows, plan.hcol)),
            shape((plan.heads, rows, rows), F32),
            shape((rows, plan.rank), F32),
            shape((rows, 1), F32),
            shape((1, plan.width), F32),
            shape((1, plan.rank), F32),
            shape((plan.half, plan.width)),
            shape((n, plan.latent, plan.wcol)),
        ],
        [
            pltpu.VMEM((n, 1, plan.wcol), F32),
            pltpu.VMEM((n, 1, plan.ccol), F32),
            pltpu.VMEM((n, rows, plan.wcol), BF16),
            pltpu.VMEM((n, rows, plan.ccol), BF16),
        ],
        5 * 10**8,
    )
    pieces = []
    for tick in range(plan.n_pipe):
        last = tick == plan.n_pipe - 1

        def backward(ranks, top, pieces, pay, v, p, chat, rc, cg, wq, wl, we, wo, cosine, sine, *outs):
            outs = list(outs)
            if not last:
                outs[2:2] = [None, None]
            backward_body(plan, last, ranks, top, pieces, pay, v, p, chat, rc, cg, wq, wl, we, wo, cosine, sine, outs)

        chunk = plan.chunk if last else plan.width
        out_groups = [[shape((plan.half, chunk))] * 2, shape((plan.half, plan.width))]
        if last:
            out_groups += [shape((rows, plan.tail)), [shape((rows, plan.wcol))] * n]
        got = kernel_call(
            backward,
            [ranks, top, pieces, pay, v, p, chat, rc, cgain32, wq, wlat, wexp, wout, cosine, sine],
            out_groups,
            [
                pltpu.VMEM((rows, plan.width), BF16),
                pltpu.VMEM((n, rows, plan.wcol), BF16),
                pltpu.VMEM((n, rows, plan.ccol), F32),
                pltpu.VMEM((n, rows, plan.wcol), BF16),
                pltpu.VMEM((rows, plan.latent + plan.spare), BF16),
            ],
            10**9,
        )
        (kept, given), up_own = got[0], got[1]
        chip = kept + exchange(given, "tensor", nt, 1)
        sums = [chip]
        for k in range(1, nt // 2):
            pairs = [(i, (i + 2 * k) % nt) for i in range(nt)]
            sums.append(lax.ppermute(chip, "tensor", pairs))
        norm_out = [shape((plan.own if last else plan.half, plan.width))]
        if last:
            tail, ups = got[2], got[3]
            norm_out.append(shape((plan.half, plan.latent + plan.spare)))

        def norm(ranks, sums, up_own, x_own, gain32, *rest):
            dx, dl, dx_s = rest if last else (rest[0], None, rest[1])
            norm_body(plan, last, ranks, sums, up_own, x_own, gain32, dx, dl, dx_s)

        got = kernel_call(
            norm,
            [ranks, sums, up_own, x_own, gain32],
            norm_out,
            [pltpu.VMEM((plan.half, plan.width), BF16)],
            10**6,
        )
        dx = got[0]
        if not last:
            below = lax.ppermute(dx, "pipe", [(s, s - 1) for s in range(1, plan.n_pipe)])
            pieces = [below, exchange(below, "tensor", nt, 1)]
    dl_own = gathered(got[1], "dp", n)
    dl_other = [exchange(block, "tensor", nt, 1) for block in dl_own]
    sent = handed(sent, "dp", n)
    pays = gathered(pay, "dp", n)
    tails = gathered(tail, "dp", n)
    ups = handed(ups, "dp", n)

    def gradients(ranks, sent, pays, tails, ups, dl_own, dl_other, cosine, sine, *outs):
        gradient_body(plan, ranks, sent, pays, tails, ups, dl_own, dl_other, cosine, sine, outs)

    every = n * rows
    g_gain, g_q, g_lat, g_lg, g_exp, g_out = kernel_call(
        gradients,
        [ranks, sent, pays, tails, ups, dl_own, dl_other, cosine, sine],
        [
            shape((1, plan.wcol), F32),
            shape((plan.wcol, plan.qcol), F32),
            shape((plan.latent, plan.wcol), F32),
            shape((1, plan.ccol), F32),
            shape((plan.ccol, plan.heads * (NOPE + VDIM)), F32),
            shape((plan.hcol, plan.wcol), F32),
        ],
        [
            pltpu.VMEM((every, plan.wcol), BF16),
            pltpu.VMEM((every, plan.ccol), BF16),
            pltpu.VMEM((every, plan.hcol), BF16),
            pltpu.VMEM((every, plan.wcol), BF16),
            pltpu.VMEM((every, plan.qcol), BF16),
            pltpu.VMEM((every, plan.heads * (NOPE + VDIM)), BF16),
            pltpu.VMEM((every, plan.latent), BF16),
            pltpu.VMEM((n, 1, plan.wcol), F32),
            pltpu.VMEM((n, 1, plan.ccol), F32),
        ],
        10**9,
    )
    results = dx.reshape(plan.micro, plan.share, plan.width)
    return results[None], g_gain, g_q[None], g_lat.T[None], g_lg, g_exp[None], g_out[None]


def shards(saved, top_grad, gain, w_query, w_latent, compressed_gain, expand_weight, w_output):
    args = (saved, top_grad, gain, w_query, w_latent, compressed_gain, expand_weight, w_output)
    sizes = [lax.axis_size(axis) for axis in ("pipe", "dp", "tensor")]
    plan = Plan(saved, w_query, w_latent, expand_weight, w_output, *sizes)
    if plan.fits():
        return token_shards(plan, *args)
    return plain_shards(*args)


def solution(mesh):
    in_specs = (
        P("pipe", None, "dp", None),
        P(None, "dp", None),
        P("pipe", "dp"),
        P("pipe", "dp", "tensor"),
        P("pipe", "dp", None),
        P("pipe", "dp"),
        P("pipe", "dp", "tensor"),
        P("pipe", "tensor", "dp"),
    )
    out_specs = (
        P("pipe", None, ("dp", "tensor"), None),
        P("pipe", "dp"),
        P("pipe", "dp", "tensor"),
        P("pipe", "dp", None),
        P("pipe", "dp"),
        P("pipe", "dp", "tensor"),
        P("pipe", "tensor", "dp"),
    )
    return jax.shard_map(shards, mesh=mesh, in_specs=in_specs, out_specs=out_specs, check_vma=False)
```

```python
import jax
import jax.numpy as jnp
import numpy as np
from jax import lax
from jax.experimental import pallas as pl
from jax.experimental.pallas import tpu as pltpu
from jax.sharding import PartitionSpec as P


NOPE = 128
ROPE = 64
VDIM = 128
COMPRESSED_RANK = 512


EPS = 1e-06


def passed_along(value, axis, steps):
    count = lax.axis_size(axis)
    first, last = (max(0, -steps), min(count, count - steps))
    return lax.ppermute(value, axis, [(source, source + steps) for source in range(first, last)])


def root_mean_scale(values, scale):
    return values * lax.rsqrt(jnp.mean(values * values, axis=-1, keepdims=True) + EPS) * scale


def rotary_angles(values):
    length = values.shape[0]
    half = values.shape[-1] // 2
    freq = jnp.exp(-jnp.log(10000.0) * jnp.arange(half, dtype=jnp.float32) / half)
    angle = jnp.arange(length, dtype=jnp.float32)[:, None] * freq[None, :]
    cosine = jnp.cos(angle)[:, None, :]
    sine = jnp.sin(angle)[:, None, :]
    first = values[..., :half]
    second = values[..., half:]
    return jnp.concatenate(
        [first * cosine - second * sine, second * cosine + first * sine], axis=-1
    )


def branch(normed, w_q, w_lat, latent_norm_gain, w_exp, w_out):
    length = normed.shape[0]
    heads = w_q.shape[1] // (NOPE + ROPE)
    rounded = normed.astype(jnp.bfloat16)
    query = jnp.dot(rounded, w_q, preferred_element_type=jnp.float32).reshape(
        length, heads, NOPE + ROPE
    )
    latent_state = jnp.dot(rounded, w_lat, preferred_element_type=jnp.float32)
    compressed_state = root_mean_scale(latent_state[:, :COMPRESSED_RANK], latent_norm_gain).astype(
        jnp.bfloat16
    )
    rotary_key_part = rotary_angles(latent_state[:, None, COMPRESSED_RANK:])[:, 0, :]
    expanded = jnp.dot(compressed_state, w_exp, preferred_element_type=jnp.float32).reshape(
        length, heads, NOPE + VDIM
    )
    key_nope = expanded[:, :, :NOPE]
    values = expanded[:, :, NOPE:].astype(jnp.bfloat16)
    query_rope = rotary_angles(query[:, :, NOPE:])
    scores = jnp.einsum("qhd,khd->hqk", query[:, :, :NOPE], key_nope) + jnp.einsum(
        "qhd,kd->hqk", query_rope, rotary_key_part
    )
    scores = scores * (NOPE + ROPE) ** (-0.5)
    causal = jnp.arange(length)[:, None] >= jnp.arange(length)[None, :]
    scores = jnp.where(causal[None], scores, -1e30)
    weights = jax.nn.softmax(scores, axis=-1).astype(jnp.bfloat16)
    mixed = jnp.einsum("hqk,khd->qhd", weights.astype(jnp.float32), values.astype(jnp.float32))
    mixed = mixed.astype(jnp.bfloat16).reshape(length, heads * VDIM)
    return jnp.dot(mixed, w_out, preferred_element_type=jnp.float32)


def plain_shards(saved, top_grad, gain, w_query, w_latent, compressed_gain, expand_weight, w_output):
    gathered = (
        lax.all_gather(gain, "dp", axis=1, tiled=True),
        lax.all_gather(w_query, "dp", axis=1, tiled=True),
        lax.all_gather(w_latent, "dp", axis=1, tiled=True),
        lax.all_gather(compressed_gain, "dp", axis=1, tiled=True),
        lax.all_gather(expand_weight, "dp", axis=1, tiled=True),
        lax.all_gather(w_output, "dp", axis=2, tiled=True),
    )
    gain32 = gathered[0][0].astype(jnp.float32)
    query_all = gathered[1][0]
    latent_all = gathered[2][0]
    lgain32 = gathered[3][0].astype(jnp.float32)
    expand_all = gathered[4][0]
    output_all = gathered[5][0]
    sections = lax.axis_size("pipe")
    section_index = lax.axis_index("pipe")
    tensor_count = lax.axis_size("tensor")
    tensor_rank = lax.axis_index("tensor")
    micro_count = saved.shape[1]
    length = saved.shape[2]
    width = saved.shape[3]
    share = length // tensor_count

    def compute(normed, upstream):
        _, pull = jax.vjp(lambda value: branch(value, query_all, latent_all, lgain32, expand_all, output_all), normed)
        return pull(upstream.astype(jnp.float32))[0]

    def skip(normed, upstream):
        return jnp.zeros_like(normed)

    gain_total = jnp.zeros((width,), jnp.float32)
    results = jnp.zeros((micro_count, share, width), jnp.bfloat16)
    stored = jnp.zeros((micro_count, length, width), jnp.bfloat16)
    received = jnp.zeros((length, width), jnp.bfloat16)
    for tick in range(sections + micro_count - 1):
        micro = tick - (sections - 1 - section_index)
        active = jnp.logical_and(micro >= 0, micro < micro_count)
        picked = jnp.clip(micro, 0, micro_count - 1)
        x_rows = lax.dynamic_index_in_dim(saved[0], picked, 0, keepdims=False)
        top_rows = lax.dynamic_index_in_dim(top_grad, picked, 0, keepdims=False)
        arrived = received
        upstream = jnp.where(section_index == sections - 1, top_rows, arrived)
        x_float = x_rows.astype(jnp.float32)
        normed, norm_pull = jax.vjp(root_mean_scale, x_float, gain32)
        branch_grad = lax.cond(active, compute, skip, normed, upstream)
        d_normed = lax.psum(branch_grad.astype(jnp.bfloat16), "tensor").astype(jnp.float32)
        dx_norm, d_gain = norm_pull(d_normed)
        dx = (upstream.astype(jnp.float32) + dx_norm).astype(jnp.bfloat16)
        gain_total = gain_total + jnp.where(active, d_gain, 0.0)
        mine = lax.dynamic_slice_in_dim(dx, tensor_rank * share, share, 0)
        chosen = (jnp.arange(micro_count) == micro)[:, None, None]
        results = jnp.where(chosen, mine[None], results)
        stored = jnp.where(chosen, upstream[None], stored)
        received = passed_along(dx, "pipe", -1)
    totals = (
        jnp.zeros(query_all.shape, jnp.float32),
        jnp.zeros(latent_all.shape, jnp.float32),
        jnp.zeros(lgain32.shape, jnp.float32),
        jnp.zeros(expand_all.shape, jnp.float32),
        jnp.zeros(output_all.shape, jnp.float32),
    )
    for micro_index in range(micro_count):
        normed_again = root_mean_scale(saved[0, micro_index].astype(jnp.float32), gain32)
        _, weight_pull = jax.vjp(
            lambda w_q, w_lat, lat_gain, w_exp, w_out: branch(
                normed_again, w_q, w_lat, lat_gain, w_exp, w_out
            ),
            query_all,
            latent_all,
            lgain32,
            expand_all,
            output_all,
        )
        cotangents = weight_pull(stored[micro_index].astype(jnp.float32))
        totals = tuple(
            (total + piece.astype(jnp.float32) for total, piece in zip(totals, cotangents))
        )
    gain_part = jnp.where(tensor_rank == 0, gain_total, 0.0)
    grad_q, grad_lat, grad_lg, grad_e, grad_o = totals
    out_q, part_lat, part_lg, out_e, out_o, part_gain = (
        lax.psum_scatter(grad_q.astype(jnp.bfloat16), "dp", scatter_dimension=0, tiled=True).astype(
            jnp.float32
        ),
        lax.psum_scatter(
            grad_lat.astype(jnp.bfloat16), "dp", scatter_dimension=0, tiled=True
        ).astype(jnp.float32),
        lax.psum_scatter(
            grad_lg.astype(jnp.bfloat16), "dp", scatter_dimension=0, tiled=True
        ).astype(jnp.float32),
        lax.psum_scatter(grad_e.astype(jnp.bfloat16), "dp", scatter_dimension=0, tiled=True).astype(
            jnp.float32
        ),
        lax.psum_scatter(grad_o.astype(jnp.bfloat16), "dp", scatter_dimension=1, tiled=True).astype(
            jnp.float32
        ),
        lax.psum_scatter(
            gain_part.astype(jnp.bfloat16), "dp", scatter_dimension=0, tiled=True
        ).astype(jnp.float32),
    )
    out_lat, out_lg, out_gain = (
        lax.psum(part_lat.astype(jnp.bfloat16), "tensor").astype(jnp.float32),
        lax.psum(part_lg.astype(jnp.bfloat16), "tensor").astype(jnp.float32),
        lax.psum(part_gain.astype(jnp.bfloat16), "tensor").astype(jnp.float32),
    )
    return (
        results[None],
        out_gain[None],
        out_q[None],
        out_lat[None],
        out_lg[None],
        out_e[None],
        out_o[None],
    )


F32 = jnp.float32
BF16 = jnp.bfloat16


def mm(a, b):
    return lax.dot_general(a, b, (((1,), (0,)), ((), ())), preferred_element_type=F32)


def mm_nt(a, b):
    return lax.dot_general(a, b, (((1,), (1,)), ((), ())), preferred_element_type=F32)


def mm_tn(a, b):
    return lax.dot_general(a, b, (((0,), (0,)), ((), ())), preferred_element_type=F32)


def turned(values):
    half = values.shape[1] // 2
    return jnp.concatenate([values[:, half:], values[:, :half]], axis=1)


def rotate(values, cosine, sine):
    return values * cosine + turned(values) * sine


def rotate_back(values, cosine, sine):
    return values * cosine - turned(values) * sine


class Plan:
    def __init__(self, saved, w_query, w_latent, expand_weight, n_pipe, n_dp, n_tensor):
        self.n_pipe, self.n, self.nt = n_pipe, n_dp, n_tensor
        self.micro, self.length, self.width = saved.shape[1:]
        self.rows = self.micro * self.length
        self.share = self.length // n_tensor
        self.heads = w_query.shape[2] // (NOPE + ROPE)
        self.rank = expand_weight.shape[1] * n_dp
        self.latent = w_latent.shape[2]
        self.wcol = self.width // n_dp
        self.ccol = self.rank // n_dp
        self.qcol = self.heads * (NOPE + ROPE)
        self.hcol = self.heads * VDIM
        self.rope_all = self.heads * ROPE
        self.o_mixed = 0
        self.o_q = self.o_mixed + self.hcol
        self.o_kn = self.o_q + self.qcol
        self.o_kr = self.o_kn + self.heads * NOPE
        self.pay = self.o_kr + ROPE
        self.o_dv = self.heads * self.length
        self.o_up = self.o_dv + self.hcol
        self.tail = self.o_up
        self.own = self.micro * self.share
        self.half = self.rows // 2
        self.spare = -self.latent % 128
        self.lrow = self.rank // max(self.spare, 1)
        self.grow = self.width // max(self.spare, 1)
        self.chunk = self.width + self.latent + self.spare

    def fits(self):
        aligned = self.wcol % 256 == 0 and self.ccol % 128 == 0 and self.rope_all % 128 == 0
        whole = (self.heads * self.length) % 128 == 0 and self.latent % 32 == 0
        if self.spare == 0 or self.rank % self.spare or self.wcol % self.spare:
            return False
        room = 2 * (self.lrow + self.grow) <= self.half
        few = self.n & (self.n - 1) == 0 and self.rows <= 512
        return aligned and whole and room and few and self.nt % 2 == 0 and self.share % 16 == 0


def share_rows(plan, core):
    at = 0
    for chip in range(plan.nt // 2):
        for m in range(plan.micro):
            start = m * plan.length + (2 * chip + core) * plan.share
            yield pl.multiple_of(start, plan.share), slice(at, at + plan.share)
            at += plan.share


def assemble_latent(plan, core, lat_own, lat_other, w_s):
    part = plan.latent // 2
    for k in range(plan.n):
        w_s[k, pl.ds(pl.multiple_of(core * part, 16), part), :] = lat_own[k][...]
        w_s[k, pl.ds(pl.multiple_of((1 - core) * part, 16), part), :] = lat_other[k][...]


def forward_body(plan, ranks, x, gains, wq, lat_own, lat_other, wexp, cosine, sine, outs):
    (sent, pay, v_ref, p_ref, chat_ref, rc_ref, gain_ref, cgain_ref, x_own, wlat, g_s, cg_s, n_s, c_s) = outs
    n = plan.n
    j, t = ranks[0], ranks[1]
    core = lax.rem(t, 2)
    assemble_latent(plan, core, lat_own, lat_other, wlat)
    for k in range(n):
        src = j ^ k
        g_s[src] = gains[k][:, : plan.wcol].astype(F32)
        cg_s[src] = gains[k][:, plan.wcol :].astype(F32)
    xf = x[...].astype(F32)
    scale = lax.rsqrt(jnp.mean(xf * xf, axis=1, keepdims=True) + EPS)
    for b in range(n):
        block = xf[:, b * plan.wcol : (b + 1) * plan.wcol] * scale * g_s[b]
        rounded = block.astype(BF16)
        n_s[b] = rounded
        gain_ref[:, b * plan.wcol : (b + 1) * plan.wcol] = g_s[b]
        cgain_ref[:, b * plan.ccol : (b + 1) * plan.ccol] = cg_s[b]
    query = jnp.zeros((plan.rows, plan.qcol), F32)
    latent = jnp.zeros((plan.rows, plan.latent), F32)
    for k in range(n):
        query = query + mm(n_s[j ^ k], wq[k][...])
        latent = latent + mm_nt(n_s[j ^ k], wlat[k])
    low = latent[:, : plan.rank]
    rc = lax.rsqrt(jnp.mean(low * low, axis=1, keepdims=True) + EPS)
    chat = low * rc
    chat_ref[...] = chat
    rc_ref[...] = rc
    comp = (chat * cgain_ref[...]).astype(BF16)
    for b in range(n):
        c_s[b] = comp[:, b * plan.ccol : (b + 1) * plan.ccol]
    expanded = jnp.zeros((plan.rows, plan.heads * (NOPE + VDIM)), F32)
    for k in range(n):
        expanded = expanded + mm(c_s[j ^ k], wexp[k][...])
    cos, sin = cosine[...], sine[...]
    kr = rotate(latent[:, plan.rank :], cos, sin).astype(BF16)
    row = lax.broadcasted_iota(jnp.int32, (plan.rows, plan.rows), 0)
    col = lax.broadcasted_iota(jnp.int32, (plan.rows, plan.rows), 1)
    keep = row >= col
    for m in range(1, plan.micro):
        keep = keep & ((row < m * plan.length) | (col >= m * plan.length))
    qn_all, qr_all, kn_all, mixed_all = [], [], [], []
    for h in range(plan.heads):
        q_at = h * (NOPE + ROPE)
        e_at = h * (NOPE + VDIM)
        qn = query[:, q_at : q_at + NOPE].astype(BF16)
        qr = rotate(query[:, q_at + NOPE : q_at + NOPE + ROPE], cos, sin).astype(BF16)
        kn = expanded[:, e_at : e_at + NOPE].astype(BF16)
        v = expanded[:, e_at + NOPE : e_at + NOPE + VDIM].astype(BF16)
        scores = (mm_nt(qn, kn) + mm_nt(qr, kr)) * (NOPE + ROPE) ** (-0.5)
        scores = jnp.where(keep, scores, -1e30)
        top = jnp.max(scores, axis=1, keepdims=True)
        e = jnp.exp(scores - top)
        p = e / jnp.sum(e, axis=1, keepdims=True)
        p_ref[h] = p
        mixed = mm(p.astype(BF16), v).astype(BF16)
        v_ref[:, h * VDIM : (h + 1) * VDIM] = v
        qn_all.append(qn)
        qr_all.append(qr)
        kn_all.append(kn)
        mixed_all.append(mixed)
    qr_cat = jnp.concatenate(qr_all, axis=1)
    for k in range(n):
        sent[k][:, : plan.wcol] = n_s[j ^ k]
        sent[k][:, plan.wcol :] = c_s[j ^ k]
    for h in range(plan.heads):
        pay[:, plan.o_mixed + h * VDIM : plan.o_mixed + (h + 1) * VDIM] = mixed_all[h]
        pay[:, plan.o_q + h * NOPE : plan.o_q + (h + 1) * NOPE] = qn_all[h]
        pay[:, plan.o_kn + h * NOPE : plan.o_kn + (h + 1) * NOPE] = kn_all[h]
    pay[:, plan.o_q + plan.heads * NOPE : plan.o_kn] = qr_cat
    pay[:, plan.o_kr :] = kr
    for start, at in share_rows(plan, core):
        x_own[at, :] = x[pl.ds(start, plan.share), :]


def key_parts(plan, pay, h):
    qn = pay[:, plan.o_q + h * NOPE : plan.o_q + (h + 1) * NOPE]
    kn = pay[:, plan.o_kn + h * NOPE : plan.o_kn + (h + 1) * NOPE]
    qr = pay[:, plan.o_q + plan.heads * NOPE : plan.o_kn][:, h * ROPE : (h + 1) * ROPE]
    return qn, kn, qr, pay[:, plan.o_kr :]


def query_cotangent(ds, kn, kr, cos, sin):
    return [mm(ds, kn).astype(BF16), rotate_back(mm(ds, kr), cos, sin).astype(BF16)]


def backward_body(plan, last, ranks, top, pieces, pay, v_ref, p_ref, chat_ref, rc_ref, cgain_ref,
                  wq, wlat, wexp, wout, cosine, sine, outs):
    chunks, up_own, tail, ups, up_s, u_s, d_s, dn_s, dl_s = outs
    n = plan.n
    j, t, is_top = ranks[0], ranks[1], ranks[2]
    core = lax.rem(t, 2)
    if pieces:
        @pl.when(is_top == 1)
        def _():
            up_s[...] = top[...]

        @pl.when(is_top == 0)
        def _():
            for piece, side in zip(pieces, (core, 1 - core)):
                for start, at in share_rows(plan, side):
                    up_s[pl.ds(start, plan.share), :] = piece[at, :]

        up_ref = up_s
    else:
        up_ref = top
    for start, at in share_rows(plan, core):
        up_own[at, :] = up_ref[pl.ds(start, plan.share), :]
    for b in range(n):
        u_s[b] = up_ref[:, b * plan.wcol : (b + 1) * plan.wcol]
    dmixed = jnp.zeros((plan.rows, plan.hcol), F32)
    for k in range(n):
        dmixed = dmixed + mm_nt(u_s[j ^ k], wout[k][...])
    dmixed = dmixed.astype(BF16)
    cos, sin = cosine[...], sine[...]
    dq, dexp, dvs, dss = [], [], [], []
    dkr = jnp.zeros((plan.rows, ROPE), F32)
    scale = (NOPE + ROPE) ** (-0.5)
    for h in range(plan.heads):
        qn, kn, qr, kr = key_parts(plan, pay, h)
        v = v_ref[:, h * VDIM : (h + 1) * VDIM]
        p = p_ref[h]
        dm = dmixed[:, h * VDIM : (h + 1) * VDIM]
        dp = mm_nt(dm, v)
        ds = (p * (dp - jnp.sum(dp * p, axis=1, keepdims=True)) * scale).astype(BF16)
        dv = mm_tn(p.astype(BF16), dm).astype(BF16)
        dq.extend(query_cotangent(ds, kn, kr, cos, sin))
        dkr = dkr + mm_tn(ds, qr)
        dexp.extend([mm_tn(ds, qn).astype(BF16), dv])
        dvs.append(dv)
        dss.append(ds)
    dq = jnp.concatenate(dq, axis=1)
    dexp = jnp.concatenate(dexp, axis=1)
    for k in range(n):
        d_s[j ^ k] = mm_nt(dexp, wexp[k][...])
    dcomp = jnp.concatenate([d_s[b] for b in range(n)], axis=1)
    chat = chat_ref[...]
    dchat = dcomp * cgain_ref[...]
    dlow = rc_ref[...] * (dchat - chat * jnp.mean(dchat * chat, axis=1, keepdims=True))
    dlatent = jnp.concatenate([dlow, rotate_back(dkr, cos, sin)], axis=1).astype(BF16)
    for k in range(n):
        dn_s[j ^ k] = (mm_nt(dq, wq[k][...]) + mm(dlatent, wlat[k])).astype(BF16)
    if last:
        dl_s[:, : plan.latent] = dlatent
        dl_s[:, plan.latent :] = jnp.zeros((plan.rows, plan.spare), BF16)
    for chunk, side in zip(chunks, (core, 1 - core)):
        for start, at in share_rows(plan, side):
            for b in range(n):
                chunk[at, b * plan.wcol : (b + 1) * plan.wcol] = dn_s[b, pl.ds(start, plan.share), :]
            if last:
                chunk[at, plan.width :] = dl_s[pl.ds(start, plan.share), :]
        if last:
            put_split(plan, chunk, plan.width + plan.latent, 0, jnp.sum(dcomp * chat, axis=0, keepdims=True))
    if last:
        small = []
        for ds in dss:
            rows = [
                ds[m * plan.length : (m + 1) * plan.length, m * plan.length : (m + 1) * plan.length]
                for m in range(plan.micro)
            ]
            small.append(jnp.concatenate(rows, axis=0))
        ds_cat = jnp.concatenate(small, axis=1)
        tail[:, : plan.o_dv] = ds_cat
        for h in range(plan.heads):
            tail[:, plan.o_dv + h * VDIM : plan.o_dv + (h + 1) * VDIM] = dvs[h]
        for k in range(n):
            ups[k][...] = u_s[j ^ k]


def put_split(plan, ref, col, row, values):
    count = values.shape[1] // plan.spare
    high = values.astype(BF16)
    low = (values - high.astype(F32)).astype(BF16)
    for i in range(count):
        piece = slice(i * plan.spare, (i + 1) * plan.spare)
        ref[row + i : row + i + 1, col : col + plan.spare] = high[:, piece]
        ref[row + count + i : row + count + i + 1, col : col + plan.spare] = low[:, piece]


def norm_body(plan, last, ranks, pieces, up_own, x_own, gain_ref, dx_ref, dl_ref, dx_s):
    total = pieces[0][...].astype(F32)
    for piece in pieces[1:]:
        total = total + piece[...].astype(F32)
    dn = total[:, : plan.width]
    x = x_own[...].astype(F32)
    scale = lax.rsqrt(jnp.mean(x * x, axis=1, keepdims=True) + EPS)
    xhat = x * scale
    dhat = dn * gain_ref[...]
    dx = scale * (dhat - xhat * jnp.mean(dhat * xhat, axis=1, keepdims=True))
    dx = (up_own[...].astype(F32) + dx).astype(BF16)
    if not last:
        dx_ref[...] = dx
        return
    dx_s[...] = dx
    at = pl.multiple_of(lax.div(ranks[1], 2) * plan.own, plan.own)
    dx_ref[...] = dx_s[pl.ds(at, plan.own), :]
    rest = total[:, plan.width :]
    dl_ref[...] = rest.astype(BF16)
    lgain = rest[: plan.lrow, plan.latent :] + rest[plan.lrow : 2 * plan.lrow, plan.latent :]
    high = lgain.astype(BF16)
    dl_ref[: plan.lrow, plan.latent :] = high
    dl_ref[plan.lrow : 2 * plan.lrow, plan.latent :] = (lgain - high.astype(F32)).astype(BF16)
    put_split(plan, dl_ref, plan.latent, 2 * plan.lrow, jnp.sum(dn * xhat, axis=0, keepdims=True))


def gradient_body(plan, sent, pays, tails, ups, cosine, sine, outs):
    g_q, g_exp, g_out, a_n, a_c, a_m, a_u, a_dq, a_de = outs
    cos, sin = cosine[...], sine[...]
    for k in range(plan.n):
        at = slice(k * plan.rows, (k + 1) * plan.rows)
        pay, tail = pays[k], tails[k]
        a_n[at, :] = sent[k][:, : plan.wcol]
        a_c[at, :] = sent[k][:, plan.wcol :]
        a_m[at, :] = pay[:, plan.o_mixed : plan.o_q]
        a_u[at, :] = ups[k][...]
        for h in range(plan.heads):
            qn, kn, _, kr = key_parts(plan, pay, h)
            for m in range(plan.micro):
                part = slice(m * plan.length, (m + 1) * plan.length)
                rows = slice(k * plan.rows + m * plan.length, k * plan.rows + (m + 1) * plan.length)
                ds = tail[part, : plan.o_dv][:, h * plan.length : (h + 1) * plan.length]
                dqn, dqr = query_cotangent(ds, kn[part], kr[part], cos[part], sin[part])
                q_at = h * (NOPE + ROPE)
                a_dq[rows, q_at : q_at + NOPE] = dqn
                a_dq[rows, q_at + NOPE : q_at + NOPE + ROPE] = dqr
                e_at = h * (NOPE + VDIM)
                a_de[rows, e_at : e_at + NOPE] = mm_tn(ds, qn[part]).astype(BF16)
                a_de[rows, e_at + NOPE : e_at + NOPE + VDIM] = tail[part, plan.o_dv + h * VDIM : plan.o_dv + (h + 1) * VDIM]
    g_q[...] = mm_tn(a_n[...], a_dq[...])
    g_exp[...] = mm_tn(a_c[...], a_de[...])
    g_out[...] = mm_tn(a_m[...], a_u[...])


def latent_gradient_body(plan, ranks, sent, dl_own, dl_other, outs):
    g_gain, g_lat, g_lg, a_n, a_dl, m_s, l_s = outs
    n = plan.n
    j, t = ranks[0], ranks[1]
    core = lax.rem(t, 2)
    lgain = jnp.zeros((plan.lrow, plan.spare), F32)
    ggain = jnp.zeros((plan.grow, plan.spare), F32)
    for k in range(n):
        a_n[k * plan.rows : (k + 1) * plan.rows, :] = sent[k][:, : plan.wcol]
        for block, side in ((dl_own[k], core), (dl_other[k], 1 - core)):
            for start, part in share_rows(plan, side):
                a_dl[pl.ds(pl.multiple_of(k * plan.rows + start, plan.share), plan.share), :] = block[part, : plan.latent]
            extra = block[:, plan.latent :].astype(F32)
            if side is core:
                lgain = lgain + extra[: plan.lrow] + extra[plan.lrow : 2 * plan.lrow]
            at_gain = 2 * plan.lrow
            ggain = ggain + extra[at_gain : at_gain + plan.grow] + extra[at_gain + plan.grow : at_gain + 2 * plan.grow]
    wide, low = plan.wcol // plan.spare, plan.ccol // plan.spare
    for b in range(n):
        for i in range(wide):
            m_s[b, :, i * plan.spare : (i + 1) * plan.spare] = ggain[b * wide + i : b * wide + i + 1, :]
        for i in range(low):
            l_s[b, :, i * plan.spare : (i + 1) * plan.spare] = lgain[b * low + i : b * low + i + 1, :]
    g_gain[...] = m_s[j]
    g_lg[...] = l_s[j]
    g_lat[...] = mm_tn(a_dl[...], a_n[...])


def grouped(counts_in, refs):
    out, at = [], 0
    for count in counts_in:
        if count is None:
            out.append(refs[at])
            at += 1
        else:
            out.append(list(refs[at : at + count]))
            at += count
    return out


def kernel_call(body, groups, out_groups, scratch, flops):
    def flat(items):
        return [leaf for item in items for leaf in (item if isinstance(item, list) else [item])]

    counts = [len(g) if isinstance(g, list) else None for g in groups + out_groups] + [None] * len(scratch)

    def kernel(*refs):
        body(*grouped(counts, refs))

    outs = flat(out_groups)
    vmem = pl.BlockSpec(memory_space=pltpu.VMEM)
    ins = flat(groups)
    call = pl.pallas_call(
        kernel,
        in_specs=[pl.BlockSpec(memory_space=pltpu.SMEM)] + [vmem] * (len(ins) - 1),
        out_specs=[vmem] * len(outs),
        out_shape=outs,
        scratch_shapes=scratch,
        compiler_params=pltpu.CompilerParams(vmem_limit_bytes=20 << 20),
        cost_estimate=pl.CostEstimate(flops=flops, bytes_accessed=4 << 20, transcendentals=0),
    )
    got = call(*ins)
    result, at = [], 0
    for g in out_groups:
        if isinstance(g, list):
            result.append(list(got[at : at + len(g)]))
            at += len(g)
        else:
            result.append(got[at])
            at += 1
    return result


def flipped(value, axis, count, bit):
    return lax.ppermute(value, axis, [(i, i ^ bit) for i in range(count)])


def gathered(value, axis, count):
    blocks = {0: value}
    bit = count // 2
    while bit:
        found = sorted(blocks)
        blocks.update({k | bit: flipped(blocks[k], axis, count, bit) for k in found})
        bit //= 2
    return [blocks[k] for k in range(count)]


def handed(values, axis, count):
    return [values[0]] + [flipped(values[k], axis, count, k) for k in range(1, count)]


def token_shards(plan, saved, top_grad, gain, w_query, w_latent, compressed_gain, expand_weight, w_output):
    n, nt, rows = plan.n, plan.nt, plan.rows
    j = lax.axis_index("dp")
    t = lax.axis_index("tensor")
    section = lax.axis_index("pipe")
    is_top = (section == plan.n_pipe - 1).astype(jnp.int32)
    ranks = jnp.stack([j, t, is_top]).astype(jnp.int32)
    part = plan.latent // 2
    half_rows = lax.dynamic_slice_in_dim(w_latent[0].T, lax.rem(t, 2) * part, part, 0)
    gains = gathered(jnp.concatenate([gain, compressed_gain], axis=1), "dp", n)
    lat_own = gathered(half_rows, "dp", n)
    lat_other = [flipped(block, "tensor", nt, 1) for block in lat_own]
    wq = gathered(w_query[0], "dp", n)
    wexp = gathered(expand_weight[0], "dp", n)
    wout = gathered(w_output[0], "dp", n)
    x = saved[0].reshape(rows, plan.width)
    top = top_grad.reshape(rows, plan.width)
    freq = 10000.0 ** (-np.arange(ROPE // 2) / (ROPE // 2))
    angle = np.tile(np.arange(plan.length)[:, None] * freq[None, :], (plan.micro, 1))
    cosine = jnp.asarray(np.concatenate([np.cos(angle), np.cos(angle)], axis=1), F32)
    sine = jnp.asarray(np.concatenate([-np.sin(angle), np.sin(angle)], axis=1), F32)

    def shape(dims, kind=BF16):
        return jax.ShapeDtypeStruct(dims, kind)

    def prepare(ranks, *refs):
        count = len(refs) // 2
        for source, target in zip(refs[:count], refs[count:]):
            target[...] = source[...]

    local = [x, top, wq[0], wexp[0], wout[0], cosine, sine]
    copied = kernel_call(prepare, [ranks] + local, [shape(v.shape, v.dtype) for v in local], [], 10**4)
    x, top, wq[0], wexp[0], wout[0], cosine, sine = copied

    def forward(ranks, x, gains, wq, lo, lt, we, cosine, sine, *outs):
        forward_body(plan, ranks, x, gains, wq, lo, lt, we, cosine, sine, outs)

    sent, pay, v, p, chat, rc, gain32, cgain32, x_own, wlat = kernel_call(
        forward,
        [ranks, x, gains, wq, lat_own, lat_other, wexp, cosine, sine],
        [
            [shape((rows, plan.wcol + plan.ccol))] * n,
            shape((rows, plan.pay)),
            shape((rows, plan.hcol)),
            shape((plan.heads, rows, rows), F32),
            shape((rows, plan.rank), F32),
            shape((rows, 1), F32),
            shape((1, plan.width), F32),
            shape((1, plan.rank), F32),
            shape((plan.half, plan.width)),
            shape((n, plan.latent, plan.wcol)),
        ],
        [
            pltpu.VMEM((n, 1, plan.wcol), F32),
            pltpu.VMEM((n, 1, plan.ccol), F32),
            pltpu.VMEM((n, rows, plan.wcol), BF16),
            pltpu.VMEM((n, rows, plan.ccol), BF16),
        ],
        5 * 10**8,
    )
    pieces = []
    for tick in range(plan.n_pipe):
        last = tick == plan.n_pipe - 1

        def backward(ranks, top, pieces, pay, v, p, chat, rc, cg, wq, wl, we, wo, cosine, sine, *outs):
            outs = list(outs)
            if not last:
                outs[2:2] = [None, None]
            backward_body(plan, last, ranks, top, pieces, pay, v, p, chat, rc, cg, wq, wl, we, wo, cosine, sine, outs)

        chunk = plan.chunk if last else plan.width
        out_groups = [[shape((plan.half, chunk))] * 2, shape((plan.half, plan.width))]
        if last:
            out_groups += [shape((rows, plan.tail)), [shape((rows, plan.wcol))] * n]
        got = kernel_call(
            backward,
            [ranks, top, pieces, pay, v, p, chat, rc, cgain32, wq, wlat, wexp, wout, cosine, sine],
            out_groups,
            [
                pltpu.VMEM((rows, plan.width), BF16),
                pltpu.VMEM((n, rows, plan.wcol), BF16),
                pltpu.VMEM((n, rows, plan.ccol), F32),
                pltpu.VMEM((n, rows, plan.wcol), BF16),
                pltpu.VMEM((rows, plan.latent + plan.spare), BF16),
            ],
            10**9,
        )
        (kept, given), up_own = got[0], got[1]
        chip = kept + flipped(given, "tensor", nt, 1)
        sums = [chip]
        for k in range(1, nt // 2):
            pairs = [(i, (i + 2 * k) % nt) for i in range(nt)]
            sums.append(lax.ppermute(chip, "tensor", pairs))
        norm_out = [shape((plan.own if last else plan.half, plan.width))]
        if last:
            tail, ups = got[2], got[3]
            norm_out.append(shape((plan.half, plan.latent + plan.spare)))

        def norm(ranks, sums, up_own, x_own, gain32, *rest):
            dx, dl, dx_s = rest if last else (rest[0], None, rest[1])
            norm_body(plan, last, ranks, sums, up_own, x_own, gain32, dx, dl, dx_s)

        got = kernel_call(
            norm, [ranks, sums, up_own, x_own, gain32], norm_out, [pltpu.VMEM((plan.half, plan.width), BF16)], 10**6
        )
        dx = got[0]
        if not last:
            below = lax.ppermute(dx, "pipe", [(s, s - 1) for s in range(1, plan.n_pipe)])
            pieces = [below, flipped(below, "tensor", nt, 1)]
    dl_own = gathered(got[1], "dp", n)
    dl_other = [flipped(block, "tensor", nt, 1) for block in dl_own]
    sent = handed(sent, "dp", n)
    pays = gathered(pay, "dp", n)
    tails = gathered(tail, "dp", n)
    ups = handed(ups, "dp", n)

    def gradients(ranks, sent, pays, tails, ups, cosine, sine, *outs):
        gradient_body(plan, sent, pays, tails, ups, cosine, sine, outs)

    def latent_gradients(ranks, sent, dl_own, dl_other, *outs):
        latent_gradient_body(plan, ranks, sent, dl_own, dl_other, outs)

    every = n * rows
    g_q, g_exp, g_out = kernel_call(
        gradients,
        [ranks, sent, pays, tails, ups, cosine, sine],
        [
            shape((plan.wcol, plan.qcol), F32),
            shape((plan.ccol, plan.heads * (NOPE + VDIM)), F32),
            shape((plan.hcol, plan.wcol), F32),
        ],
        [
            pltpu.VMEM((every, plan.wcol), BF16),
            pltpu.VMEM((every, plan.ccol), BF16),
            pltpu.VMEM((every, plan.hcol), BF16),
            pltpu.VMEM((every, plan.wcol), BF16),
            pltpu.VMEM((every, plan.qcol), BF16),
            pltpu.VMEM((every, plan.heads * (NOPE + VDIM)), BF16),
        ],
        10**9,
    )
    g_gain, g_lat, g_lg = kernel_call(
        latent_gradients,
        [ranks, sent, dl_own, dl_other],
        [shape((1, plan.wcol), F32), shape((plan.latent, plan.wcol), F32), shape((1, plan.ccol), F32)],
        [
            pltpu.VMEM((every, plan.wcol), BF16),
            pltpu.VMEM((every, plan.latent), BF16),
            pltpu.VMEM((n, 1, plan.wcol), F32),
            pltpu.VMEM((n, 1, plan.ccol), F32),
        ],
        10**9,
    )
    results = dx.reshape(plan.micro, plan.share, plan.width)
    return results[None], g_gain, g_q[None], g_lat.T[None], g_lg, g_exp[None], g_out[None]


def shards(saved, top_grad, gain, w_query, w_latent, compressed_gain, expand_weight, w_output):
    args = (saved, top_grad, gain, w_query, w_latent, compressed_gain, expand_weight, w_output)
    sizes = [lax.axis_size(axis) for axis in ("pipe", "dp", "tensor")]
    plan = Plan(saved, w_query, w_latent, expand_weight, *sizes)
    if plan.fits():
        return token_shards(plan, *args)
    return plain_shards(*args)


def solution(mesh):
    in_specs = (
        P("pipe", None, "dp", None),
        P(None, "dp", None),
        P("pipe", "dp"),
        P("pipe", "dp", "tensor"),
        P("pipe", "dp", None),
        P("pipe", "dp"),
        P("pipe", "dp", "tensor"),
        P("pipe", "tensor", "dp"),
    )
    out_specs = (
        P("pipe", None, ("dp", "tensor"), None),
        P("pipe", "dp"),
        P("pipe", "dp", "tensor"),
        P("pipe", "dp", None),
        P("pipe", "dp"),
        P("pipe", "dp", "tensor"),
        P("pipe", "tensor", "dp"),
    )
    return jax.shard_map(shards, mesh=mesh, in_specs=in_specs, out_specs=out_specs, check_vma=False)
```

```python
import jax
import jax.numpy as jnp
import numpy as np
from jax import lax
from jax.experimental import pallas as pl
from jax.experimental.pallas import tpu as pltpu
from jax.sharding import PartitionSpec as P


NOPE = 128
ROPE = 64
VDIM = 128
COMPRESSED_RANK = 512


EPS = 1e-06


def passed_along(value, axis, steps):
    count = lax.axis_size(axis)
    first, last = (max(0, -steps), min(count, count - steps))
    return lax.ppermute(value, axis, [(source, source + steps) for source in range(first, last)])


def root_mean_scale(values, scale):
    return values * lax.rsqrt(jnp.mean(values * values, axis=-1, keepdims=True) + EPS) * scale


def rotary_angles(values):
    length = values.shape[0]
    half = values.shape[-1] // 2
    freq = jnp.exp(-jnp.log(10000.0) * jnp.arange(half, dtype=jnp.float32) / half)
    angle = jnp.arange(length, dtype=jnp.float32)[:, None] * freq[None, :]
    cosine = jnp.cos(angle)[:, None, :]
    sine = jnp.sin(angle)[:, None, :]
    first = values[..., :half]
    second = values[..., half:]
    return jnp.concatenate(
        [first * cosine - second * sine, second * cosine + first * sine], axis=-1
    )


def branch(normed, w_q, w_lat, latent_norm_gain, w_exp, w_out):
    length = normed.shape[0]
    heads = w_q.shape[1] // (NOPE + ROPE)
    rounded = normed.astype(jnp.bfloat16)
    query = jnp.dot(rounded, w_q, preferred_element_type=jnp.float32).reshape(
        length, heads, NOPE + ROPE
    )
    latent_state = jnp.dot(rounded, w_lat, preferred_element_type=jnp.float32)
    compressed_state = root_mean_scale(latent_state[:, :COMPRESSED_RANK], latent_norm_gain).astype(
        jnp.bfloat16
    )
    rotary_key_part = rotary_angles(latent_state[:, None, COMPRESSED_RANK:])[:, 0, :]
    expanded = jnp.dot(compressed_state, w_exp, preferred_element_type=jnp.float32).reshape(
        length, heads, NOPE + VDIM
    )
    key_nope = expanded[:, :, :NOPE]
    values = expanded[:, :, NOPE:].astype(jnp.bfloat16)
    query_rope = rotary_angles(query[:, :, NOPE:])
    scores = jnp.einsum("qhd,khd->hqk", query[:, :, :NOPE], key_nope) + jnp.einsum(
        "qhd,kd->hqk", query_rope, rotary_key_part
    )
    scores = scores * (NOPE + ROPE) ** (-0.5)
    causal = jnp.arange(length)[:, None] >= jnp.arange(length)[None, :]
    scores = jnp.where(causal[None], scores, -1e30)
    weights = jax.nn.softmax(scores, axis=-1).astype(jnp.bfloat16)
    mixed = jnp.einsum("hqk,khd->qhd", weights.astype(jnp.float32), values.astype(jnp.float32))
    mixed = mixed.astype(jnp.bfloat16).reshape(length, heads * VDIM)
    return jnp.dot(mixed, w_out, preferred_element_type=jnp.float32)


def plain_shards(saved, top_grad, gain, w_query, w_latent, compressed_gain, expand_weight, w_output):
    gathered = (
        lax.all_gather(gain, "dp", axis=1, tiled=True),
        lax.all_gather(w_query, "dp", axis=1, tiled=True),
        lax.all_gather(w_latent, "dp", axis=1, tiled=True),
        lax.all_gather(compressed_gain, "dp", axis=1, tiled=True),
        lax.all_gather(expand_weight, "dp", axis=1, tiled=True),
        lax.all_gather(w_output, "dp", axis=2, tiled=True),
    )
    gain32 = gathered[0][0].astype(jnp.float32)
    query_all = gathered[1][0]
    latent_all = gathered[2][0]
    lgain32 = gathered[3][0].astype(jnp.float32)
    expand_all = gathered[4][0]
    output_all = gathered[5][0]
    sections = lax.axis_size("pipe")
    section_index = lax.axis_index("pipe")
    tensor_count = lax.axis_size("tensor")
    tensor_rank = lax.axis_index("tensor")
    micro_count = saved.shape[1]
    length = saved.shape[2]
    width = saved.shape[3]
    share = length // tensor_count

    def compute(normed, upstream):
        _, pull = jax.vjp(lambda value: branch(value, query_all, latent_all, lgain32, expand_all, output_all), normed)
        return pull(upstream.astype(jnp.float32))[0]

    def skip(normed, upstream):
        return jnp.zeros_like(normed)

    gain_total = jnp.zeros((width,), jnp.float32)
    results = jnp.zeros((micro_count, share, width), jnp.bfloat16)
    stored = jnp.zeros((micro_count, length, width), jnp.bfloat16)
    received = jnp.zeros((length, width), jnp.bfloat16)
    for tick in range(sections + micro_count - 1):
        micro = tick - (sections - 1 - section_index)
        active = jnp.logical_and(micro >= 0, micro < micro_count)
        picked = jnp.clip(micro, 0, micro_count - 1)
        x_rows = lax.dynamic_index_in_dim(saved[0], picked, 0, keepdims=False)
        top_rows = lax.dynamic_index_in_dim(top_grad, picked, 0, keepdims=False)
        arrived = received
        upstream = jnp.where(section_index == sections - 1, top_rows, arrived)
        x_float = x_rows.astype(jnp.float32)
        normed, norm_pull = jax.vjp(root_mean_scale, x_float, gain32)
        branch_grad = lax.cond(active, compute, skip, normed, upstream)
        d_normed = lax.psum(branch_grad.astype(jnp.bfloat16), "tensor").astype(jnp.float32)
        dx_norm, d_gain = norm_pull(d_normed)
        dx = (upstream.astype(jnp.float32) + dx_norm).astype(jnp.bfloat16)
        gain_total = gain_total + jnp.where(active, d_gain, 0.0)
        mine = lax.dynamic_slice_in_dim(dx, tensor_rank * share, share, 0)
        chosen = (jnp.arange(micro_count) == micro)[:, None, None]
        results = jnp.where(chosen, mine[None], results)
        stored = jnp.where(chosen, upstream[None], stored)
        received = passed_along(dx, "pipe", -1)
    totals = (
        jnp.zeros(query_all.shape, jnp.float32),
        jnp.zeros(latent_all.shape, jnp.float32),
        jnp.zeros(lgain32.shape, jnp.float32),
        jnp.zeros(expand_all.shape, jnp.float32),
        jnp.zeros(output_all.shape, jnp.float32),
    )
    for micro_index in range(micro_count):
        normed_again = root_mean_scale(saved[0, micro_index].astype(jnp.float32), gain32)
        _, weight_pull = jax.vjp(
            lambda w_q, w_lat, lat_gain, w_exp, w_out: branch(
                normed_again, w_q, w_lat, lat_gain, w_exp, w_out
            ),
            query_all,
            latent_all,
            lgain32,
            expand_all,
            output_all,
        )
        cotangents = weight_pull(stored[micro_index].astype(jnp.float32))
        totals = tuple(
            (total + piece.astype(jnp.float32) for total, piece in zip(totals, cotangents))
        )
    gain_part = jnp.where(tensor_rank == 0, gain_total, 0.0)
    grad_q, grad_lat, grad_lg, grad_e, grad_o = totals
    out_q, part_lat, part_lg, out_e, out_o, part_gain = (
        lax.psum_scatter(grad_q.astype(jnp.bfloat16), "dp", scatter_dimension=0, tiled=True).astype(
            jnp.float32
        ),
        lax.psum_scatter(
            grad_lat.astype(jnp.bfloat16), "dp", scatter_dimension=0, tiled=True
        ).astype(jnp.float32),
        lax.psum_scatter(
            grad_lg.astype(jnp.bfloat16), "dp", scatter_dimension=0, tiled=True
        ).astype(jnp.float32),
        lax.psum_scatter(grad_e.astype(jnp.bfloat16), "dp", scatter_dimension=0, tiled=True).astype(
            jnp.float32
        ),
        lax.psum_scatter(grad_o.astype(jnp.bfloat16), "dp", scatter_dimension=1, tiled=True).astype(
            jnp.float32
        ),
        lax.psum_scatter(
            gain_part.astype(jnp.bfloat16), "dp", scatter_dimension=0, tiled=True
        ).astype(jnp.float32),
    )
    out_lat, out_lg, out_gain = (
        lax.psum(part_lat.astype(jnp.bfloat16), "tensor").astype(jnp.float32),
        lax.psum(part_lg.astype(jnp.bfloat16), "tensor").astype(jnp.float32),
        lax.psum(part_gain.astype(jnp.bfloat16), "tensor").astype(jnp.float32),
    )
    return (
        results[None],
        out_gain[None],
        out_q[None],
        out_lat[None],
        out_lg[None],
        out_e[None],
        out_o[None],
    )


F32 = jnp.float32
BF16 = jnp.bfloat16


def mm(a, b):
    return lax.dot_general(a, b, (((1,), (0,)), ((), ())), preferred_element_type=F32)


def mm_nt(a, b):
    return lax.dot_general(a, b, (((1,), (1,)), ((), ())), preferred_element_type=F32)


def mm_tn(a, b):
    return lax.dot_general(a, b, (((0,), (0,)), ((), ())), preferred_element_type=F32)


def turned(values):
    half = values.shape[1] // 2
    return jnp.concatenate([values[:, half:], values[:, :half]], axis=1)


def rotate(values, cosine, sine):
    return values * cosine + turned(values) * sine


def rotate_back(values, cosine, sine):
    return values * cosine - turned(values) * sine


class Plan:
    def __init__(self, saved, w_query, w_latent, expand_weight, n_pipe, n_dp, n_tensor):
        self.n_pipe, self.n, self.nt = n_pipe, n_dp, n_tensor
        self.micro, self.length, self.width = saved.shape[1:]
        self.rows = self.micro * self.length
        self.share = self.length // n_tensor
        self.heads = w_query.shape[2] // (NOPE + ROPE)
        self.rank = expand_weight.shape[1] * n_dp
        self.latent = w_latent.shape[2]
        self.wcol = self.width // n_dp
        self.ccol = self.rank // n_dp
        self.qcol = self.heads * (NOPE + ROPE)
        self.hcol = self.heads * VDIM
        self.rope_all = self.heads * ROPE
        self.o_mixed = 0
        self.o_q = self.o_mixed + self.hcol
        self.o_kn = self.o_q + self.qcol
        self.o_kr = self.o_kn + self.heads * NOPE
        self.pay = self.o_kr + ROPE
        self.o_dv = self.heads * self.length
        self.o_up = self.o_dv + self.hcol
        self.tail = self.o_up
        self.own = self.micro * self.share
        self.half = self.rows // 2
        self.part = self.latent // n_tensor
        self.spare = -self.latent % 128
        self.lrow = self.rank // max(self.spare, 1)
        self.grow = self.width // max(self.spare, 1)
        self.chunk = self.width + self.latent + self.spare

    def fits(self):
        aligned = self.wcol % 256 == 0 and self.ccol % 128 == 0 and self.rope_all % 128 == 0
        whole = (self.heads * self.length) % 128 == 0 and self.latent % (16 * self.nt) == 0
        if self.spare == 0 or self.rank % self.spare or self.wcol % self.spare:
            return False
        room = 2 * (self.lrow + self.grow) <= self.half
        few = self.n & (self.n - 1) == 0 and self.nt & (self.nt - 1) == 0 and self.rows <= 512
        return aligned and whole and room and few and self.nt % 2 == 0 and self.share % 16 == 0


def share_rows(plan, core):
    at = 0
    for chip in range(plan.nt // 2):
        for m in range(plan.micro):
            start = m * plan.length + (2 * chip + core) * plan.share
            yield pl.multiple_of(start, plan.share), slice(at, at + plan.share)
            at += plan.share


def piece_body(plan, ranks, w_lat, gain, cgain, piece):
    at = pl.multiple_of(ranks[1] * plan.part, 16)
    piece[: plan.part, :] = w_lat[pl.ds(at, plan.part), :]
    piece[plan.part : plan.part + 1, :] = gain[...]
    piece[plan.part + 1 : plan.part + 2, : plan.ccol] = cgain[...]


def assemble_latent(plan, t, lat, w_s):
    for k in range(plan.n):
        for i in range(plan.nt):
            to = pl.ds(pl.multiple_of((t ^ i) * plan.part, 16), plan.part)
            w_s[k, to, :] = lat[i][k * (plan.part + 16) : k * (plan.part + 16) + plan.part, :]


def forward_body(plan, ranks, x, wq, lat, wexp, table, outs):
    (sent, pay, v_ref, p_ref, chat_ref, rc_ref, gain_ref, cgain_ref, x_own, wlat, g_s, cg_s, n_s, c_s) = outs
    n = plan.n
    j, t = ranks[0], ranks[1]
    core = lax.rem(t, 2)
    assemble_latent(plan, t, lat, wlat)
    for k in range(n):
        src = j ^ k
        both = lat[0][k * (plan.part + 16) + plan.part : (k + 1) * (plan.part + 16), :].astype(F32)
        g_s[src] = both[:1]
        cg_s[src] = both[1:2, : plan.ccol]
    xf = x[...].astype(F32)
    scale = lax.rsqrt(jnp.mean(xf * xf, axis=1, keepdims=True) + EPS)
    for b in range(n):
        block = xf[:, b * plan.wcol : (b + 1) * plan.wcol] * scale * g_s[b]
        rounded = block.astype(BF16)
        n_s[b] = rounded
        gain_ref[:, b * plan.wcol : (b + 1) * plan.wcol] = g_s[b]
        cgain_ref[:, b * plan.ccol : (b + 1) * plan.ccol] = cg_s[b]
    query = jnp.zeros((plan.rows, plan.qcol), F32)
    latent = jnp.zeros((plan.rows, plan.latent), F32)
    for k in range(n):
        query = query + mm(n_s[j ^ k], wq[k][...])
        latent = latent + mm_nt(n_s[j ^ k], wlat[k])
    low = latent[:, : plan.rank]
    rc = lax.rsqrt(jnp.mean(low * low, axis=1, keepdims=True) + EPS)
    chat = low * rc
    chat_ref[...] = chat
    rc_ref[...] = rc
    comp = (chat * cgain_ref[...]).astype(BF16)
    for b in range(n):
        c_s[b] = comp[:, b * plan.ccol : (b + 1) * plan.ccol]
    expanded = jnp.zeros((plan.rows, plan.heads * (NOPE + VDIM)), F32)
    for k in range(n):
        expanded = expanded + mm(c_s[j ^ k], wexp[k][...])
    cos, sin = table[:, :ROPE], table[:, ROPE:]
    kr = rotate(latent[:, plan.rank :], cos, sin).astype(BF16)
    row = lax.broadcasted_iota(jnp.int32, (plan.rows, plan.rows), 0)
    col = lax.broadcasted_iota(jnp.int32, (plan.rows, plan.rows), 1)
    keep = row >= col
    for m in range(1, plan.micro):
        keep = keep & ((row < m * plan.length) | (col >= m * plan.length))
    qn_all, qr_all, kn_all, mixed_all = [], [], [], []
    for h in range(plan.heads):
        q_at = h * (NOPE + ROPE)
        e_at = h * (NOPE + VDIM)
        qn = query[:, q_at : q_at + NOPE].astype(BF16)
        qr = rotate(query[:, q_at + NOPE : q_at + NOPE + ROPE], cos, sin).astype(BF16)
        kn = expanded[:, e_at : e_at + NOPE].astype(BF16)
        v = expanded[:, e_at + NOPE : e_at + NOPE + VDIM].astype(BF16)
        scores = (mm_nt(qn, kn) + mm_nt(qr, kr)) * (NOPE + ROPE) ** (-0.5)
        scores = jnp.where(keep, scores, -1e30)
        top = jnp.max(scores, axis=1, keepdims=True)
        e = jnp.exp(scores - top)
        p = e / jnp.sum(e, axis=1, keepdims=True)
        p_ref[h] = p
        mixed = mm(p.astype(BF16), v).astype(BF16)
        v_ref[:, h * VDIM : (h + 1) * VDIM] = v
        qn_all.append(qn)
        qr_all.append(qr)
        kn_all.append(kn)
        mixed_all.append(mixed)
    qr_cat = jnp.concatenate(qr_all, axis=1)
    for k in range(n):
        for start, at in share_rows(plan, core):
            sent[k][at, : plan.wcol] = n_s[j ^ k, pl.ds(start, plan.share), :]
            sent[k][at, plan.wcol :] = c_s[j ^ k, pl.ds(start, plan.share), :]
    for h in range(plan.heads):
        pay[:, plan.o_mixed + h * VDIM : plan.o_mixed + (h + 1) * VDIM] = mixed_all[h]
        pay[:, plan.o_q + h * NOPE : plan.o_q + (h + 1) * NOPE] = qn_all[h]
        pay[:, plan.o_kn + h * NOPE : plan.o_kn + (h + 1) * NOPE] = kn_all[h]
    pay[:, plan.o_q + plan.heads * NOPE : plan.o_kn] = qr_cat
    pay[:, plan.o_kr :] = kr
    for start, at in share_rows(plan, core):
        x_own[at, :] = x[pl.ds(start, plan.share), :]


def key_parts(plan, pay, h):
    qn = pay[:, plan.o_q + h * NOPE : plan.o_q + (h + 1) * NOPE]
    kn = pay[:, plan.o_kn + h * NOPE : plan.o_kn + (h + 1) * NOPE]
    qr = pay[:, plan.o_q + plan.heads * NOPE : plan.o_kn][:, h * ROPE : (h + 1) * ROPE]
    return qn, kn, qr, pay[:, plan.o_kr :]


def query_cotangent(ds, kn, kr, cos, sin):
    return [mm(ds, kn).astype(BF16), rotate_back(mm(ds, kr), cos, sin).astype(BF16)]


def backward_body(plan, last, ranks, top, pieces, pay, v_ref, p_ref, chat_ref, rc_ref, cgain_ref,
                  wq, wlat, wexp, wout, table, outs):
    chunks, up_own, tail, ups, up_s, u_s, d_s, dn_s, dl_s = outs
    n = plan.n
    j, t, is_top = ranks[0], ranks[1], ranks[2]
    core = lax.rem(t, 2)
    if pieces:
        @pl.when(is_top == 1)
        def _():
            up_s[...] = top[...]

        @pl.when(is_top == 0)
        def _():
            for piece, side in zip(pieces, (core, 1 - core)):
                for start, at in share_rows(plan, side):
                    up_s[pl.ds(start, plan.share), :] = piece[at, :]

        up_ref = up_s
    else:
        up_ref = top
    for start, at in share_rows(plan, core):
        up_own[at, :] = up_ref[pl.ds(start, plan.share), :]
    for b in range(n):
        u_s[b] = up_ref[:, b * plan.wcol : (b + 1) * plan.wcol]
    dmixed = jnp.zeros((plan.rows, plan.hcol), F32)
    for k in range(n):
        dmixed = dmixed + mm_nt(u_s[j ^ k], wout[k][...])
    dmixed = dmixed.astype(BF16)
    cos, sin = table[:, :ROPE], table[:, ROPE:]
    dq, dexp, dvs, dss = [], [], [], []
    dkr = jnp.zeros((plan.rows, ROPE), F32)
    scale = (NOPE + ROPE) ** (-0.5)
    for h in range(plan.heads):
        qn, kn, qr, kr = key_parts(plan, pay, h)
        v = v_ref[:, h * VDIM : (h + 1) * VDIM]
        p = p_ref[h]
        dm = dmixed[:, h * VDIM : (h + 1) * VDIM]
        dp = mm_nt(dm, v)
        ds = (p * (dp - jnp.sum(dp * p, axis=1, keepdims=True)) * scale).astype(BF16)
        dv = mm_tn(p.astype(BF16), dm).astype(BF16)
        dq.extend(query_cotangent(ds, kn, kr, cos, sin))
        dkr = dkr + mm_tn(ds, qr)
        dexp.extend([mm_tn(ds, qn).astype(BF16), dv])
        dvs.append(dv)
        dss.append(ds)
    dq = jnp.concatenate(dq, axis=1)
    dexp = jnp.concatenate(dexp, axis=1)
    for k in range(n):
        d_s[j ^ k] = mm_nt(dexp, wexp[k][...])
    dcomp = jnp.concatenate([d_s[b] for b in range(n)], axis=1)
    chat = chat_ref[...]
    dchat = dcomp * cgain_ref[...]
    dlow = rc_ref[...] * (dchat - chat * jnp.mean(dchat * chat, axis=1, keepdims=True))
    dlatent = jnp.concatenate([dlow, rotate_back(dkr, cos, sin)], axis=1).astype(BF16)
    for k in range(n):
        dn_s[j ^ k] = (mm_nt(dq, wq[k][...]) + mm(dlatent, wlat[k])).astype(BF16)
    if last:
        dl_s[:, : plan.latent] = dlatent
        dl_s[:, plan.latent :] = jnp.zeros((plan.rows, plan.spare), BF16)
    for chunk, side in zip(chunks, (core, 1 - core)):
        for start, at in share_rows(plan, side):
            for b in range(n):
                chunk[at, b * plan.wcol : (b + 1) * plan.wcol] = dn_s[b, pl.ds(start, plan.share), :]
            if last:
                chunk[at, plan.width :] = dl_s[pl.ds(start, plan.share), :]
        if last:
            put_split(plan, chunk, plan.width + plan.latent, 0, jnp.sum(dcomp * chat, axis=0, keepdims=True))
    if last:
        small = []
        for ds in dss:
            rows = [
                ds[m * plan.length : (m + 1) * plan.length, m * plan.length : (m + 1) * plan.length]
                for m in range(plan.micro)
            ]
            small.append(jnp.concatenate(rows, axis=0))
        ds_cat = jnp.concatenate(small, axis=1)
        tail[:, : plan.o_dv] = ds_cat
        for h in range(plan.heads):
            tail[:, plan.o_dv + h * VDIM : plan.o_dv + (h + 1) * VDIM] = dvs[h]
        for k in range(n):
            for start, at in share_rows(plan, core):
                ups[k][at, :] = u_s[j ^ k, pl.ds(start, plan.share), :]


def put_split(plan, ref, col, row, values):
    count = values.shape[1] // plan.spare
    high = values.astype(BF16)
    low = (values - high.astype(F32)).astype(BF16)
    for i in range(count):
        piece = slice(i * plan.spare, (i + 1) * plan.spare)
        ref[row + i : row + i + 1, col : col + plan.spare] = high[:, piece]
        ref[row + count + i : row + count + i + 1, col : col + plan.spare] = low[:, piece]


def norm_body(plan, last, ranks, pieces, up_own, x_own, gain_ref, dx_ref, dl_ref, dx_s):
    total = pieces[0][...].astype(F32)
    for piece in pieces[1:]:
        total = total + piece[...].astype(F32)
    dn = total[:, : plan.width]
    x = x_own[...].astype(F32)
    scale = lax.rsqrt(jnp.mean(x * x, axis=1, keepdims=True) + EPS)
    xhat = x * scale
    dhat = dn * gain_ref[...]
    dx = scale * (dhat - xhat * jnp.mean(dhat * xhat, axis=1, keepdims=True))
    dx = (up_own[...].astype(F32) + dx).astype(BF16)
    if not last:
        dx_ref[...] = dx
        return
    dx_s[...] = dx
    at = pl.multiple_of(lax.div(ranks[1], 2) * plan.own, plan.own)
    dx_ref[...] = dx_s[pl.ds(at, plan.own), :]
    rest = total[:, plan.width :]
    dl_ref[...] = rest.astype(BF16)
    lgain = rest[: plan.lrow, plan.latent :] + rest[plan.lrow : 2 * plan.lrow, plan.latent :]
    high = lgain.astype(BF16)
    dl_ref[: plan.lrow, plan.latent :] = high
    dl_ref[plan.lrow : 2 * plan.lrow, plan.latent :] = (lgain - high.astype(F32)).astype(BF16)
    put_split(plan, dl_ref, plan.latent, 2 * plan.lrow, jnp.sum(dn * xhat, axis=0, keepdims=True))


def gradient_body(plan, ranks, sent, sent_o, pays, tails, table, outs):
    g_q, g_exp, a_n, a_c, a_dq, a_de = outs
    cos, sin = table[:, :ROPE], table[:, ROPE:]
    core = lax.rem(ranks[1], 2)
    for k in range(plan.n):
        pay, tail = pays[k], tails[k]
        for side, block in ((core, sent[k]), (1 - core, sent_o[k])):
            for start, part in share_rows(plan, side):
                to = pl.ds(pl.multiple_of(k * plan.rows + start, plan.share), plan.share)
                a_n[to, :] = block[part, : plan.wcol]
                a_c[to, :] = block[part, plan.wcol :]
        for h in range(plan.heads):
            qn, kn, _, kr = key_parts(plan, pay, h)
            for m in range(plan.micro):
                part = slice(m * plan.length, (m + 1) * plan.length)
                rows = slice(k * plan.rows + m * plan.length, k * plan.rows + (m + 1) * plan.length)
                ds = tail[part, : plan.o_dv][:, h * plan.length : (h + 1) * plan.length]
                dqn, dqr = query_cotangent(ds, kn[part], kr[part], cos[part], sin[part])
                q_at = h * (NOPE + ROPE)
                a_dq[rows, q_at : q_at + NOPE] = dqn
                a_dq[rows, q_at + NOPE : q_at + NOPE + ROPE] = dqr
                e_at = h * (NOPE + VDIM)
                a_de[rows, e_at : e_at + NOPE] = mm_tn(ds, qn[part]).astype(BF16)
                a_de[rows, e_at + NOPE : e_at + NOPE + VDIM] = tail[part, plan.o_dv + h * VDIM : plan.o_dv + (h + 1) * VDIM]
    g_q[...] = mm_tn(a_n[...], a_dq[...])
    g_exp[...] = mm_tn(a_c[...], a_de[...])


def latent_gradient_body(plan, ranks, sent, sent_o, pays, ups, ups_o, dl_own, dl_other, outs):
    g_gain, g_lat, g_lg, g_out, a_n, a_m, a_u, a_dl, m_s, l_s = outs
    n = plan.n
    j, t = ranks[0], ranks[1]
    core = lax.rem(t, 2)
    lgain = jnp.zeros((plan.lrow, plan.spare), F32)
    ggain = jnp.zeros((plan.grow, plan.spare), F32)
    for k in range(n):
        a_m[k * plan.rows : (k + 1) * plan.rows, :] = pays[k][:, plan.o_mixed : plan.o_q]
        mine, theirs = (dl_own[k], sent[k], ups[k], core), (dl_other[k], sent_o[k], ups_o[k], 1 - core)
        for block, rows, up, side in (mine, theirs):
            for start, part in share_rows(plan, side):
                to = pl.ds(pl.multiple_of(k * plan.rows + start, plan.share), plan.share)
                a_n[to, :] = rows[part, : plan.wcol]
                a_u[to, :] = up[part, :]
                a_dl[pl.ds(pl.multiple_of(k * plan.rows + start, plan.share), plan.share), :] = block[part, : plan.latent]
            extra = block[:, plan.latent :].astype(F32)
            if side is core:
                lgain = lgain + extra[: plan.lrow] + extra[plan.lrow : 2 * plan.lrow]
            at_gain = 2 * plan.lrow
            ggain = ggain + extra[at_gain : at_gain + plan.grow] + extra[at_gain + plan.grow : at_gain + 2 * plan.grow]
    wide, low = plan.wcol // plan.spare, plan.ccol // plan.spare
    for b in range(n):
        for i in range(wide):
            m_s[b, :, i * plan.spare : (i + 1) * plan.spare] = ggain[b * wide + i : b * wide + i + 1, :]
        for i in range(low):
            l_s[b, :, i * plan.spare : (i + 1) * plan.spare] = lgain[b * low + i : b * low + i + 1, :]
    g_gain[...] = m_s[j]
    g_lg[...] = l_s[j]
    g_lat[...] = mm_tn(a_dl[...], a_n[...])
    g_out[...] = mm_tn(a_m[...], a_u[...])


def grouped(counts_in, refs):
    out, at = [], 0
    for count in counts_in:
        if count is None:
            out.append(refs[at])
            at += 1
        else:
            out.append(list(refs[at : at + count]))
            at += count
    return out


def kernel_call(body, groups, out_groups, scratch, flops):
    def flat(items):
        return [leaf for item in items for leaf in (item if isinstance(item, list) else [item])]

    counts = [len(g) if isinstance(g, list) else None for g in groups + out_groups] + [None] * len(scratch)

    def kernel(*refs):
        body(*grouped(counts, refs))

    outs = flat(out_groups)
    vmem = pl.BlockSpec(memory_space=pltpu.VMEM)
    ins = flat(groups)
    call = pl.pallas_call(
        kernel,
        in_specs=[pl.BlockSpec(memory_space=pltpu.SMEM)] + [vmem] * (len(ins) - 1),
        out_specs=[vmem] * len(outs),
        out_shape=outs,
        scratch_shapes=scratch,
        compiler_params=pltpu.CompilerParams(vmem_limit_bytes=20 << 20),
        cost_estimate=pl.CostEstimate(flops=flops, bytes_accessed=4 << 20, transcendentals=0),
    )
    got = call(*ins)
    result, at = [], 0
    for g in out_groups:
        if isinstance(g, list):
            result.append(list(got[at : at + len(g)]))
            at += len(g)
        else:
            result.append(got[at])
            at += 1
    return result


def flipped(value, axis, count, bit):
    return lax.ppermute(value, axis, [(i, i ^ bit) for i in range(count)])


def gathered(value, axis, count):
    blocks = {0: value}
    bit = count // 2
    while bit:
        found = sorted(blocks)
        blocks.update({k | bit: flipped(blocks[k], axis, count, bit) for k in found})
        bit //= 2
    return [blocks[k] for k in range(count)]


def handed(values, axis, count):
    return [values[0]] + [flipped(values[k], axis, count, k) for k in range(1, count)]


def token_shards(plan, saved, top_grad, gain, w_query, w_latent, compressed_gain, expand_weight, w_output):
    n, nt, rows = plan.n, plan.nt, plan.rows
    j = lax.axis_index("dp")
    t = lax.axis_index("tensor")
    section = lax.axis_index("pipe")
    is_top = (section == plan.n_pipe - 1).astype(jnp.int32)
    ranks = jnp.stack([j, t, is_top]).astype(jnp.int32)

    def shape(dims, kind=BF16):
        return jax.ShapeDtypeStruct(dims, kind)

    def pick(ranks, w_lat, gain, cgain, piece):
        piece_body(plan, ranks, w_lat, gain, cgain, piece)

    def stack(ranks, blocks, target):
        for k, block in enumerate(blocks):
            target[k * (plan.part + 16) : (k + 1) * (plan.part + 16), :] = block[...]

    tall = plan.part + 16
    (piece,) = kernel_call(pick, [ranks, w_latent[0].T, gain, compressed_gain], [shape((tall, plan.wcol))], [], 10**4)
    blocks = gathered(piece, "dp", n)
    (stacked,) = kernel_call(stack, [ranks, blocks], [shape((n * tall, plan.wcol))], [], 10**4)
    lat = gathered(stacked, "tensor", nt)
    wq = gathered(w_query[0], "dp", n)
    wexp = gathered(expand_weight[0], "dp", n)
    wout = gathered(w_output[0], "dp", n)
    x = saved[0].reshape(rows, plan.width)
    top = top_grad.reshape(rows, plan.width)
    freq = 10000.0 ** (-np.arange(ROPE // 2) / (ROPE // 2))
    angle = np.tile(np.arange(plan.length)[:, None] * freq[None, :], (plan.micro, 1))
    cos, sin = np.cos(angle), np.sin(angle)
    table = jnp.asarray(np.concatenate([cos, cos, -sin, sin], axis=1), F32)

    def prepare(ranks, *refs):
        count = len(refs) // 2
        for source, target in zip(refs[:count], refs[count:]):
            target[...] = source[...]

    def local(values):
        shapes = [shape(v.shape, v.dtype) for v in values]
        return kernel_call(prepare, [ranks] + values, shapes, [], 10**4)

    x, wq[0], wexp[0], table = local([x, wq[0], wexp[0], table])
    top, wout[0] = local([top, wout[0]])

    def forward(ranks, x, wq, lat, we, table, *outs):
        forward_body(plan, ranks, x, wq, lat, we, table, outs)

    sent, pay, v, p, chat, rc, gain32, cgain32, x_own, wlat = kernel_call(
        forward,
        [ranks, x, wq, lat, wexp, table],
        [
            [shape((plan.half, plan.wcol + plan.ccol))] * n,
            shape((rows, plan.pay)),
            shape((rows, plan.hcol)),
            shape((plan.heads, rows, rows), F32),
            shape((rows, plan.rank), F32),
            shape((rows, 1), F32),
            shape((1, plan.width), F32),
            shape((1, plan.rank), F32),
            shape((plan.half, plan.width)),
            shape((n, plan.latent, plan.wcol)),
        ],
        [
            pltpu.VMEM((n, 1, plan.wcol), F32),
            pltpu.VMEM((n, 1, plan.ccol), F32),
            pltpu.VMEM((n, rows, plan.wcol), BF16),
            pltpu.VMEM((n, rows, plan.ccol), BF16),
        ],
        5 * 10**8,
    )
    pieces = []
    for tick in range(plan.n_pipe):
        last = tick == plan.n_pipe - 1

        def backward(ranks, top, pieces, pay, v, p, chat, rc, cg, wq, wl, we, wo, table, *outs):
            outs = list(outs)
            if not last:
                outs[2:2] = [None, None]
            backward_body(plan, last, ranks, top, pieces, pay, v, p, chat, rc, cg, wq, wl, we, wo, table, outs)

        chunk = plan.chunk if last else plan.width
        out_groups = [[shape((plan.half, chunk))] * 2, shape((plan.half, plan.width))]
        if last:
            out_groups += [shape((rows, plan.tail)), [shape((plan.half, plan.wcol))] * n]
        got = kernel_call(
            backward,
            [ranks, top, pieces, pay, v, p, chat, rc, cgain32, wq, wlat, wexp, wout, table],
            out_groups,
            [
                pltpu.VMEM((rows, plan.width), BF16),
                pltpu.VMEM((n, rows, plan.wcol), BF16),
                pltpu.VMEM((n, rows, plan.ccol), F32),
                pltpu.VMEM((n, rows, plan.wcol), BF16),
                pltpu.VMEM((rows, plan.latent + plan.spare), BF16),
            ],
            10**9,
        )
        (kept, given), up_own = got[0], got[1]
        chip = kept + flipped(given, "tensor", nt, 1)
        sums = [chip]
        for k in range(1, nt // 2):
            pairs = [(i, (i + 2 * k) % nt) for i in range(nt)]
            sums.append(lax.ppermute(chip, "tensor", pairs))
        norm_out = [shape((plan.own if last else plan.half, plan.width))]
        if last:
            tail, ups = got[2], got[3]
            norm_out.append(shape((plan.half, plan.latent + plan.spare)))

        def norm(ranks, sums, up_own, x_own, gain32, *rest):
            dx, dl, dx_s = rest if last else (rest[0], None, rest[1])
            norm_body(plan, last, ranks, sums, up_own, x_own, gain32, dx, dl, dx_s)

        got = kernel_call(
            norm, [ranks, sums, up_own, x_own, gain32], norm_out, [pltpu.VMEM((plan.half, plan.width), BF16)], 10**6
        )
        dx = got[0]
        if not last:
            below = lax.ppermute(dx, "pipe", [(s, s - 1) for s in range(1, plan.n_pipe)])
            pieces = [below, flipped(below, "tensor", nt, 1)]
    dl_own = gathered(got[1], "dp", n)
    dl_other = [flipped(block, "tensor", nt, 1) for block in dl_own]
    sent = handed(sent, "dp", n)
    sent_o = [flipped(block, "tensor", nt, 1) for block in sent]
    pays = gathered(pay, "dp", n)
    tails = gathered(tail, "dp", n)
    ups = handed(ups, "dp", n)
    ups_o = [flipped(block, "tensor", nt, 1) for block in ups]

    def gradients(ranks, sent, sent_o, pays, tails, table, *outs):
        gradient_body(plan, ranks, sent, sent_o, pays, tails, table, outs)

    def latent_gradients(ranks, sent, sent_o, pays, ups, ups_o, dl_own, dl_other, *outs):
        latent_gradient_body(plan, ranks, sent, sent_o, pays, ups, ups_o, dl_own, dl_other, outs)

    every = n * rows
    g_q, g_exp = kernel_call(
        gradients,
        [ranks, sent, sent_o, pays, tails, table],
        [shape((plan.wcol, plan.qcol), F32), shape((plan.ccol, plan.heads * (NOPE + VDIM)), F32)],
        [
            pltpu.VMEM((every, plan.wcol), BF16),
            pltpu.VMEM((every, plan.ccol), BF16),
            pltpu.VMEM((every, plan.qcol), BF16),
            pltpu.VMEM((every, plan.heads * (NOPE + VDIM)), BF16),
        ],
        10**9,
    )
    g_gain, g_lat, g_lg, g_out = kernel_call(
        latent_gradients,
        [ranks, sent, sent_o, pays, ups, ups_o, dl_own, dl_other],
        [
            shape((1, plan.wcol), F32),
            shape((plan.latent, plan.wcol), F32),
            shape((1, plan.ccol), F32),
            shape((plan.hcol, plan.wcol), F32),
        ],
        [
            pltpu.VMEM((every, plan.wcol), BF16),
            pltpu.VMEM((every, plan.hcol), BF16),
            pltpu.VMEM((every, plan.wcol), BF16),
            pltpu.VMEM((every, plan.latent), BF16),
            pltpu.VMEM((n, 1, plan.wcol), F32),
            pltpu.VMEM((n, 1, plan.ccol), F32),
        ],
        10**9,
    )
    results = dx.reshape(plan.micro, plan.share, plan.width)
    return results[None], g_gain, g_q[None], g_lat.T[None], g_lg, g_exp[None], g_out[None]


def shards(saved, top_grad, gain, w_query, w_latent, compressed_gain, expand_weight, w_output):
    args = (saved, top_grad, gain, w_query, w_latent, compressed_gain, expand_weight, w_output)
    sizes = [lax.axis_size(axis) for axis in ("pipe", "dp", "tensor")]
    plan = Plan(saved, w_query, w_latent, expand_weight, *sizes)
    if plan.fits():
        return token_shards(plan, *args)
    return plain_shards(*args)


def solution(mesh):
    in_specs = (
        P("pipe", None, "dp", None),
        P(None, "dp", None),
        P("pipe", "dp"),
        P("pipe", "dp", "tensor"),
        P("pipe", "dp", None),
        P("pipe", "dp"),
        P("pipe", "dp", "tensor"),
        P("pipe", "tensor", "dp"),
    )
    out_specs = (
        P("pipe", None, ("dp", "tensor"), None),
        P("pipe", "dp"),
        P("pipe", "dp", "tensor"),
        P("pipe", "dp", None),
        P("pipe", "dp"),
        P("pipe", "dp", "tensor"),
        P("pipe", "tensor", "dp"),
    )
    return jax.shard_map(shards, mesh=mesh, in_specs=in_specs, out_specs=out_specs, check_vma=False)
```

```python
import jax
import jax.numpy as jnp
import numpy as np
from jax import lax
from jax.experimental import pallas as pl
from jax.experimental.pallas import tpu as pltpu
from jax.sharding import PartitionSpec as P


NOPE = 128
ROPE = 64
VDIM = 128
COMPRESSED_RANK = 512


EPS = 1e-06


def passed_along(value, axis, steps):
    count = lax.axis_size(axis)
    first, last = (max(0, -steps), min(count, count - steps))
    return lax.ppermute(value, axis, [(source, source + steps) for source in range(first, last)])


def root_mean_scale(values, scale):
    return values * lax.rsqrt(jnp.mean(values * values, axis=-1, keepdims=True) + EPS) * scale


def rotary_angles(values):
    length = values.shape[0]
    half = values.shape[-1] // 2
    freq = jnp.exp(-jnp.log(10000.0) * jnp.arange(half, dtype=jnp.float32) / half)
    angle = jnp.arange(length, dtype=jnp.float32)[:, None] * freq[None, :]
    cosine = jnp.cos(angle)[:, None, :]
    sine = jnp.sin(angle)[:, None, :]
    first = values[..., :half]
    second = values[..., half:]
    return jnp.concatenate(
        [first * cosine - second * sine, second * cosine + first * sine], axis=-1
    )


def branch(normed, w_q, w_lat, latent_norm_gain, w_exp, w_out):
    length = normed.shape[0]
    heads = w_q.shape[1] // (NOPE + ROPE)
    rounded = normed.astype(jnp.bfloat16)
    query = jnp.dot(rounded, w_q, preferred_element_type=jnp.float32).reshape(
        length, heads, NOPE + ROPE
    )
    latent_state = jnp.dot(rounded, w_lat, preferred_element_type=jnp.float32)
    compressed_state = root_mean_scale(latent_state[:, :COMPRESSED_RANK], latent_norm_gain).astype(
        jnp.bfloat16
    )
    rotary_key_part = rotary_angles(latent_state[:, None, COMPRESSED_RANK:])[:, 0, :]
    expanded = jnp.dot(compressed_state, w_exp, preferred_element_type=jnp.float32).reshape(
        length, heads, NOPE + VDIM
    )
    key_nope = expanded[:, :, :NOPE]
    values = expanded[:, :, NOPE:].astype(jnp.bfloat16)
    query_rope = rotary_angles(query[:, :, NOPE:])
    scores = jnp.einsum("qhd,khd->hqk", query[:, :, :NOPE], key_nope) + jnp.einsum(
        "qhd,kd->hqk", query_rope, rotary_key_part
    )
    scores = scores * (NOPE + ROPE) ** (-0.5)
    causal = jnp.arange(length)[:, None] >= jnp.arange(length)[None, :]
    scores = jnp.where(causal[None], scores, -1e30)
    weights = jax.nn.softmax(scores, axis=-1).astype(jnp.bfloat16)
    mixed = jnp.einsum("hqk,khd->qhd", weights.astype(jnp.float32), values.astype(jnp.float32))
    mixed = mixed.astype(jnp.bfloat16).reshape(length, heads * VDIM)
    return jnp.dot(mixed, w_out, preferred_element_type=jnp.float32)


def plain_shards(saved, top_grad, gain, w_query, w_latent, compressed_gain, expand_weight, w_output):
    gathered = (
        lax.all_gather(gain, "dp", axis=1, tiled=True),
        lax.all_gather(w_query, "dp", axis=1, tiled=True),
        lax.all_gather(w_latent, "dp", axis=1, tiled=True),
        lax.all_gather(compressed_gain, "dp", axis=1, tiled=True),
        lax.all_gather(expand_weight, "dp", axis=1, tiled=True),
        lax.all_gather(w_output, "dp", axis=2, tiled=True),
    )
    gain32 = gathered[0][0].astype(jnp.float32)
    query_all = gathered[1][0]
    latent_all = gathered[2][0]
    lgain32 = gathered[3][0].astype(jnp.float32)
    expand_all = gathered[4][0]
    output_all = gathered[5][0]
    sections = lax.axis_size("pipe")
    section_index = lax.axis_index("pipe")
    tensor_count = lax.axis_size("tensor")
    tensor_rank = lax.axis_index("tensor")
    micro_count = saved.shape[1]
    length = saved.shape[2]
    width = saved.shape[3]
    share = length // tensor_count

    def compute(normed, upstream):
        _, pull = jax.vjp(lambda value: branch(value, query_all, latent_all, lgain32, expand_all, output_all), normed)
        return pull(upstream.astype(jnp.float32))[0]

    def skip(normed, upstream):
        return jnp.zeros_like(normed)

    gain_total = jnp.zeros((width,), jnp.float32)
    results = jnp.zeros((micro_count, share, width), jnp.bfloat16)
    stored = jnp.zeros((micro_count, length, width), jnp.bfloat16)
    received = jnp.zeros((length, width), jnp.bfloat16)
    for tick in range(sections + micro_count - 1):
        micro = tick - (sections - 1 - section_index)
        active = jnp.logical_and(micro >= 0, micro < micro_count)
        picked = jnp.clip(micro, 0, micro_count - 1)
        x_rows = lax.dynamic_index_in_dim(saved[0], picked, 0, keepdims=False)
        top_rows = lax.dynamic_index_in_dim(top_grad, picked, 0, keepdims=False)
        arrived = received
        upstream = jnp.where(section_index == sections - 1, top_rows, arrived)
        x_float = x_rows.astype(jnp.float32)
        normed, norm_pull = jax.vjp(root_mean_scale, x_float, gain32)
        branch_grad = lax.cond(active, compute, skip, normed, upstream)
        d_normed = lax.psum(branch_grad.astype(jnp.bfloat16), "tensor").astype(jnp.float32)
        dx_norm, d_gain = norm_pull(d_normed)
        dx = (upstream.astype(jnp.float32) + dx_norm).astype(jnp.bfloat16)
        gain_total = gain_total + jnp.where(active, d_gain, 0.0)
        mine = lax.dynamic_slice_in_dim(dx, tensor_rank * share, share, 0)
        chosen = (jnp.arange(micro_count) == micro)[:, None, None]
        results = jnp.where(chosen, mine[None], results)
        stored = jnp.where(chosen, upstream[None], stored)
        received = passed_along(dx, "pipe", -1)
    totals = (
        jnp.zeros(query_all.shape, jnp.float32),
        jnp.zeros(latent_all.shape, jnp.float32),
        jnp.zeros(lgain32.shape, jnp.float32),
        jnp.zeros(expand_all.shape, jnp.float32),
        jnp.zeros(output_all.shape, jnp.float32),
    )
    for micro_index in range(micro_count):
        normed_again = root_mean_scale(saved[0, micro_index].astype(jnp.float32), gain32)
        _, weight_pull = jax.vjp(
            lambda w_q, w_lat, lat_gain, w_exp, w_out: branch(
                normed_again, w_q, w_lat, lat_gain, w_exp, w_out
            ),
            query_all,
            latent_all,
            lgain32,
            expand_all,
            output_all,
        )
        cotangents = weight_pull(stored[micro_index].astype(jnp.float32))
        totals = tuple(
            (total + piece.astype(jnp.float32) for total, piece in zip(totals, cotangents))
        )
    gain_part = jnp.where(tensor_rank == 0, gain_total, 0.0)
    grad_q, grad_lat, grad_lg, grad_e, grad_o = totals
    out_q, part_lat, part_lg, out_e, out_o, part_gain = (
        lax.psum_scatter(grad_q.astype(jnp.bfloat16), "dp", scatter_dimension=0, tiled=True).astype(
            jnp.float32
        ),
        lax.psum_scatter(
            grad_lat.astype(jnp.bfloat16), "dp", scatter_dimension=0, tiled=True
        ).astype(jnp.float32),
        lax.psum_scatter(
            grad_lg.astype(jnp.bfloat16), "dp", scatter_dimension=0, tiled=True
        ).astype(jnp.float32),
        lax.psum_scatter(grad_e.astype(jnp.bfloat16), "dp", scatter_dimension=0, tiled=True).astype(
            jnp.float32
        ),
        lax.psum_scatter(grad_o.astype(jnp.bfloat16), "dp", scatter_dimension=1, tiled=True).astype(
            jnp.float32
        ),
        lax.psum_scatter(
            gain_part.astype(jnp.bfloat16), "dp", scatter_dimension=0, tiled=True
        ).astype(jnp.float32),
    )
    out_lat, out_lg, out_gain = (
        lax.psum(part_lat.astype(jnp.bfloat16), "tensor").astype(jnp.float32),
        lax.psum(part_lg.astype(jnp.bfloat16), "tensor").astype(jnp.float32),
        lax.psum(part_gain.astype(jnp.bfloat16), "tensor").astype(jnp.float32),
    )
    return (
        results[None],
        out_gain[None],
        out_q[None],
        out_lat[None],
        out_lg[None],
        out_e[None],
        out_o[None],
    )


F32 = jnp.float32
BF16 = jnp.bfloat16


def mm(a, b):
    return lax.dot_general(a, b, (((1,), (0,)), ((), ())), preferred_element_type=F32)


def mm_nt(a, b):
    return lax.dot_general(a, b, (((1,), (1,)), ((), ())), preferred_element_type=F32)


def mm_tn(a, b):
    return lax.dot_general(a, b, (((0,), (0,)), ((), ())), preferred_element_type=F32)


def turned(values):
    half = values.shape[1] // 2
    return jnp.concatenate([values[:, half:], values[:, :half]], axis=1)


def rotate(values, cosine, sine):
    return values * cosine + turned(values) * sine


def rotate_back(values, cosine, sine):
    return values * cosine - turned(values) * sine


class Plan:
    def __init__(self, saved, w_query, w_latent, expand_weight, n_pipe, n_dp, n_tensor):
        self.n_pipe, self.n, self.nt = n_pipe, n_dp, n_tensor
        self.micro, self.length, self.width = saved.shape[1:]
        self.rows = self.micro * self.length
        self.share = self.length // n_tensor
        self.heads = w_query.shape[2] // (NOPE + ROPE)
        self.rank = expand_weight.shape[1] * n_dp
        self.latent = w_latent.shape[2]
        self.wcol = self.width // n_dp
        self.ccol = self.rank // n_dp
        self.qcol = self.heads * (NOPE + ROPE)
        self.hcol = self.heads * VDIM
        self.rope_all = self.heads * ROPE
        self.o_mixed = 0
        self.o_q = self.o_mixed + self.hcol
        self.o_kn = self.o_q + self.qcol
        self.o_kr = self.o_kn + self.heads * NOPE
        self.pay = self.o_kr + ROPE
        self.o_dv = self.heads * self.length
        self.o_up = self.o_dv + self.hcol
        self.tail = self.o_up
        self.own = self.micro * self.share
        self.half = self.rows // 2
        self.part = self.latent // n_tensor
        self.spare = -self.latent % 128
        self.lrow = self.rank // max(self.spare, 1)
        self.grow = self.width // max(self.spare, 1)
        self.chunk = self.width + self.latent + self.spare

    def fits(self):
        aligned = self.wcol % 256 == 0 and self.ccol % 128 == 0 and self.rope_all % 128 == 0
        whole = (self.heads * self.length) % 128 == 0 and self.latent % (16 * self.nt) == 0
        if self.spare == 0 or self.rank % self.spare or self.wcol % self.spare:
            return False
        room = 2 * (self.lrow + self.grow) <= self.half
        few = self.n & (self.n - 1) == 0 and self.nt & (self.nt - 1) == 0 and self.rows <= 512
        return aligned and whole and room and few and self.nt % 2 == 0 and self.share % 16 == 0


def share_rows(plan, core):
    at = 0
    for chip in range(plan.nt // 2):
        for m in range(plan.micro):
            start = m * plan.length + (2 * chip + core) * plan.share
            yield pl.multiple_of(start, plan.share), slice(at, at + plan.share)
            at += plan.share


def piece_body(plan, ranks, w_lat, gain, cgain, piece, gain_s, cgain_s, sems):
    at = pl.multiple_of(ranks[1] * plan.part, 16)
    moves = [
        pltpu.make_async_copy(w_lat.at[pl.ds(at, plan.part), :], piece.at[pl.ds(0, plan.part), :], sems.at[0]),
        pltpu.make_async_copy(gain, gain_s, sems.at[1]),
        pltpu.make_async_copy(cgain, cgain_s, sems.at[2]),
    ]
    for move in moves:
        move.start()
    for move in moves:
        move.wait()
    piece[plan.part : plan.part + 1, :] = gain_s[...]
    piece[plan.part + 1 : plan.part + 2, : plan.ccol] = cgain_s[...]


def assemble_latent(plan, t, lat, w_s):
    for k in range(plan.n):
        for i in range(plan.nt):
            to = pl.ds(pl.multiple_of((t ^ i) * plan.part, 16), plan.part)
            w_s[k, to, :] = lat[i][k * (plan.part + 16) : k * (plan.part + 16) + plan.part, :]


def forward_body(plan, ranks, x, wq, lat, wexp, table, outs):
    (sent, pay, v_ref, p_ref, chat_ref, rc_ref, gain_ref, cgain_ref, wlat, g_s, cg_s, n_s, c_s) = outs
    n = plan.n
    j, t = ranks[0], ranks[1]
    core = lax.rem(t, 2)
    assemble_latent(plan, t, lat, wlat)
    for k in range(n):
        src = j ^ k
        both = lat[0][k * (plan.part + 16) + plan.part : (k + 1) * (plan.part + 16), :].astype(F32)
        g_s[src] = both[:1]
        cg_s[src] = both[1:2, : plan.ccol]
    xf = x[...].astype(F32)
    scale = lax.rsqrt(jnp.mean(xf * xf, axis=1, keepdims=True) + EPS)
    for b in range(n):
        block = xf[:, b * plan.wcol : (b + 1) * plan.wcol] * scale * g_s[b]
        rounded = block.astype(BF16)
        n_s[b] = rounded
        gain_ref[:, b * plan.wcol : (b + 1) * plan.wcol] = g_s[b]
        cgain_ref[:, b * plan.ccol : (b + 1) * plan.ccol] = cg_s[b]
    query = jnp.zeros((plan.rows, plan.qcol), F32)
    latent = jnp.zeros((plan.rows, plan.latent), F32)
    for k in range(n):
        query = query + mm(n_s[j ^ k], wq[k][...])
        latent = latent + mm_nt(n_s[j ^ k], wlat[k])
    low = latent[:, : plan.rank]
    rc = lax.rsqrt(jnp.mean(low * low, axis=1, keepdims=True) + EPS)
    chat = low * rc
    chat_ref[...] = chat
    rc_ref[...] = rc
    comp = (chat * cgain_ref[...]).astype(BF16)
    for b in range(n):
        c_s[b] = comp[:, b * plan.ccol : (b + 1) * plan.ccol]
    expanded = jnp.zeros((plan.rows, plan.heads * (NOPE + VDIM)), F32)
    for k in range(n):
        expanded = expanded + mm(c_s[j ^ k], wexp[k][...])
    cos, sin = table[:, :ROPE], table[:, ROPE:]
    kr = rotate(latent[:, plan.rank :], cos, sin).astype(BF16)
    row = lax.broadcasted_iota(jnp.int32, (plan.rows, plan.rows), 0)
    col = lax.broadcasted_iota(jnp.int32, (plan.rows, plan.rows), 1)
    keep = row >= col
    for m in range(1, plan.micro):
        keep = keep & ((row < m * plan.length) | (col >= m * plan.length))
    qn_all, qr_all, kn_all, mixed_all = [], [], [], []
    for h in range(plan.heads):
        q_at = h * (NOPE + ROPE)
        e_at = h * (NOPE + VDIM)
        qn = query[:, q_at : q_at + NOPE].astype(BF16)
        qr = rotate(query[:, q_at + NOPE : q_at + NOPE + ROPE], cos, sin).astype(BF16)
        kn = expanded[:, e_at : e_at + NOPE].astype(BF16)
        v = expanded[:, e_at + NOPE : e_at + NOPE + VDIM].astype(BF16)
        scores = (mm_nt(qn, kn) + mm_nt(qr, kr)) * (NOPE + ROPE) ** (-0.5)
        scores = jnp.where(keep, scores, -1e30)
        top = jnp.max(scores, axis=1, keepdims=True)
        e = jnp.exp(scores - top)
        p = e / jnp.sum(e, axis=1, keepdims=True)
        p_ref[h] = p
        mixed = mm(p.astype(BF16), v).astype(BF16)
        v_ref[:, h * VDIM : (h + 1) * VDIM] = v
        qn_all.append(qn)
        qr_all.append(qr)
        kn_all.append(kn)
        mixed_all.append(mixed)
    qr_cat = jnp.concatenate(qr_all, axis=1)
    for k in range(n):
        for start, at in share_rows(plan, core):
            sent[k][at, : plan.wcol] = n_s[j ^ k, pl.ds(start, plan.share), :]
            sent[k][at, plan.wcol :] = c_s[j ^ k, pl.ds(start, plan.share), :]
    for h in range(plan.heads):
        pay[:, plan.o_mixed + h * VDIM : plan.o_mixed + (h + 1) * VDIM] = mixed_all[h]
        pay[:, plan.o_q + h * NOPE : plan.o_q + (h + 1) * NOPE] = qn_all[h]
        pay[:, plan.o_kn + h * NOPE : plan.o_kn + (h + 1) * NOPE] = kn_all[h]
    pay[:, plan.o_q + plan.heads * NOPE : plan.o_kn] = qr_cat
    pay[:, plan.o_kr :] = kr


def key_parts(plan, pay, h):
    qn = pay[:, plan.o_q + h * NOPE : plan.o_q + (h + 1) * NOPE]
    kn = pay[:, plan.o_kn + h * NOPE : plan.o_kn + (h + 1) * NOPE]
    qr = pay[:, plan.o_q + plan.heads * NOPE : plan.o_kn][:, h * ROPE : (h + 1) * ROPE]
    return qn, kn, qr, pay[:, plan.o_kr :]


def query_cotangent(ds, kn, kr, cos, sin):
    return [mm(ds, kn).astype(BF16), rotate_back(mm(ds, kr), cos, sin).astype(BF16)]


def backward_body(plan, last, ranks, top, pieces, pay, v_ref, p_ref, chat_ref, rc_ref, cgain_ref,
                  wq, wlat, wexp, wout, table, outs):
    chunks, up_own, tail, ups, up_s, u_s, d_s, dn_s, dl_s = outs
    n = plan.n
    j, t, is_top = ranks[0], ranks[1], ranks[2]
    core = lax.rem(t, 2)
    if pieces:
        @pl.when(is_top == 1)
        def _():
            up_s[...] = top[...]

        @pl.when(is_top == 0)
        def _():
            for piece, side in zip(pieces, (core, 1 - core)):
                for start, at in share_rows(plan, side):
                    up_s[pl.ds(start, plan.share), :] = piece[at, :]

        up_ref = up_s
    else:
        up_ref = top
    for start, at in share_rows(plan, core):
        up_own[at, :] = up_ref[pl.ds(start, plan.share), :]
    for b in range(n):
        u_s[b] = up_ref[:, b * plan.wcol : (b + 1) * plan.wcol]
    dmixed = jnp.zeros((plan.rows, plan.hcol), F32)
    for k in range(n):
        dmixed = dmixed + mm_nt(u_s[j ^ k], wout[k][...])
    dmixed = dmixed.astype(BF16)
    cos, sin = table[:, :ROPE], table[:, ROPE:]
    dq, dexp, dvs, dss = [], [], [], []
    dkr = jnp.zeros((plan.rows, ROPE), F32)
    scale = (NOPE + ROPE) ** (-0.5)
    for h in range(plan.heads):
        qn, kn, qr, kr = key_parts(plan, pay, h)
        v = v_ref[:, h * VDIM : (h + 1) * VDIM]
        p = p_ref[h]
        dm = dmixed[:, h * VDIM : (h + 1) * VDIM]
        dp = mm_nt(dm, v)
        ds = (p * (dp - jnp.sum(dp * p, axis=1, keepdims=True)) * scale).astype(BF16)
        dv = mm_tn(p.astype(BF16), dm).astype(BF16)
        dq.extend(query_cotangent(ds, kn, kr, cos, sin))
        dkr = dkr + mm_tn(ds, qr)
        dexp.extend([mm_tn(ds, qn).astype(BF16), dv])
        dvs.append(dv)
        dss.append(ds)
    dq = jnp.concatenate(dq, axis=1)
    dexp = jnp.concatenate(dexp, axis=1)
    for k in range(n):
        d_s[j ^ k] = mm_nt(dexp, wexp[k][...])
    dcomp = jnp.concatenate([d_s[b] for b in range(n)], axis=1)
    chat = chat_ref[...]
    dchat = dcomp * cgain_ref[...]
    dlow = rc_ref[...] * (dchat - chat * jnp.mean(dchat * chat, axis=1, keepdims=True))
    dlatent = jnp.concatenate([dlow, rotate_back(dkr, cos, sin)], axis=1).astype(BF16)
    for k in range(n):
        dn_s[j ^ k] = (mm_nt(dq, wq[k][...]) + mm(dlatent, wlat[k])).astype(BF16)
    if last:
        dl_s[:, : plan.latent] = dlatent
        dl_s[:, plan.latent :] = jnp.zeros((plan.rows, plan.spare), BF16)
    for chunk, side in zip(chunks, (core, 1 - core)):
        for start, at in share_rows(plan, side):
            for b in range(n):
                chunk[at, b * plan.wcol : (b + 1) * plan.wcol] = dn_s[b, pl.ds(start, plan.share), :]
            if last:
                chunk[at, plan.width :] = dl_s[pl.ds(start, plan.share), :]
        if last:
            put_split(plan, chunk, plan.width + plan.latent, 0, jnp.sum(dcomp * chat, axis=0, keepdims=True))
    if last:
        small = []
        for ds in dss:
            rows = [
                ds[m * plan.length : (m + 1) * plan.length, m * plan.length : (m + 1) * plan.length]
                for m in range(plan.micro)
            ]
            small.append(jnp.concatenate(rows, axis=0))
        ds_cat = jnp.concatenate(small, axis=1)
        tail[:, : plan.o_dv] = ds_cat
        for h in range(plan.heads):
            tail[:, plan.o_dv + h * VDIM : plan.o_dv + (h + 1) * VDIM] = dvs[h]
        for k in range(n):
            for start, at in share_rows(plan, core):
                ups[k][at, :] = u_s[j ^ k, pl.ds(start, plan.share), :]


def put_split(plan, ref, col, row, values):
    count = values.shape[1] // plan.spare
    high = values.astype(BF16)
    low = (values - high.astype(F32)).astype(BF16)
    for i in range(count):
        piece = slice(i * plan.spare, (i + 1) * plan.spare)
        ref[row + i : row + i + 1, col : col + plan.spare] = high[:, piece]
        ref[row + count + i : row + count + i + 1, col : col + plan.spare] = low[:, piece]


def norm_body(plan, last, ranks, pieces, up_own, x_own, gain_ref, dx_ref, dl_ref, dx_s):
    total = pieces[0][...].astype(F32)
    for piece in pieces[1:]:
        total = total + piece[...].astype(F32)
    dn = total[:, : plan.width]
    x = x_own[...].astype(F32)
    scale = lax.rsqrt(jnp.mean(x * x, axis=1, keepdims=True) + EPS)
    xhat = x * scale
    dhat = dn * gain_ref[...]
    dx = scale * (dhat - xhat * jnp.mean(dhat * xhat, axis=1, keepdims=True))
    dx = (up_own[...].astype(F32) + dx).astype(BF16)
    if not last:
        dx_ref[...] = dx
        return
    dx_s[...] = dx
    at = pl.multiple_of(lax.div(ranks[1], 2) * plan.own, plan.own)
    dx_ref[...] = dx_s[pl.ds(at, plan.own), :]
    rest = total[:, plan.width :]
    dl_ref[...] = rest.astype(BF16)
    lgain = rest[: plan.lrow, plan.latent :] + rest[plan.lrow : 2 * plan.lrow, plan.latent :]
    high = lgain.astype(BF16)
    dl_ref[: plan.lrow, plan.latent :] = high
    dl_ref[plan.lrow : 2 * plan.lrow, plan.latent :] = (lgain - high.astype(F32)).astype(BF16)
    put_split(plan, dl_ref, plan.latent, 2 * plan.lrow, jnp.sum(dn * xhat, axis=0, keepdims=True))


def gradient_body(plan, ranks, sent, sent_o, pays, tails, table, outs):
    g_q, g_exp, a_n, a_c, a_dq, a_de = outs
    cos, sin = table[:, :ROPE], table[:, ROPE:]
    core = lax.rem(ranks[1], 2)
    for k in range(plan.n):
        pay, tail = pays[k], tails[k]
        for side, block in ((core, sent[k]), (1 - core, sent_o[k])):
            for start, part in share_rows(plan, side):
                to = pl.ds(pl.multiple_of(k * plan.rows + start, plan.share), plan.share)
                a_n[to, :] = block[part, : plan.wcol]
                a_c[to, :] = block[part, plan.wcol :]
        for h in range(plan.heads):
            qn, kn, _, kr = key_parts(plan, pay, h)
            for m in range(plan.micro):
                part = slice(m * plan.length, (m + 1) * plan.length)
                rows = slice(k * plan.rows + m * plan.length, k * plan.rows + (m + 1) * plan.length)
                ds = tail[part, : plan.o_dv][:, h * plan.length : (h + 1) * plan.length]
                dqn, dqr = query_cotangent(ds, kn[part], kr[part], cos[part], sin[part])
                q_at = h * (NOPE + ROPE)
                a_dq[rows, q_at : q_at + NOPE] = dqn
                a_dq[rows, q_at + NOPE : q_at + NOPE + ROPE] = dqr
                e_at = h * (NOPE + VDIM)
                a_de[rows, e_at : e_at + NOPE] = mm_tn(ds, qn[part]).astype(BF16)
                a_de[rows, e_at + NOPE : e_at + NOPE + VDIM] = tail[part, plan.o_dv + h * VDIM : plan.o_dv + (h + 1) * VDIM]
    g_q[...] = mm_tn(a_n[...], a_dq[...])
    g_exp[...] = mm_tn(a_c[...], a_de[...])


def latent_gradient_body(plan, ranks, sent, sent_o, pays, ups, ups_o, dl_own, dl_other, outs):
    g_gain, g_lat, g_lg, g_out, a_n, a_m, a_u, a_dl, m_s, l_s = outs
    n = plan.n
    j, t = ranks[0], ranks[1]
    core = lax.rem(t, 2)
    lgain = jnp.zeros((plan.lrow, plan.spare), F32)
    ggain = jnp.zeros((plan.grow, plan.spare), F32)
    for k in range(n):
        a_m[k * plan.rows : (k + 1) * plan.rows, :] = pays[k][:, plan.o_mixed : plan.o_q]
        mine, theirs = (dl_own[k], sent[k], ups[k], core), (dl_other[k], sent_o[k], ups_o[k], 1 - core)
        for block, rows, up, side in (mine, theirs):
            for start, part in share_rows(plan, side):
                to = pl.ds(pl.multiple_of(k * plan.rows + start, plan.share), plan.share)
                a_n[to, :] = rows[part, : plan.wcol]
                a_u[to, :] = up[part, :]
                a_dl[pl.ds(pl.multiple_of(k * plan.rows + start, plan.share), plan.share), :] = block[part, : plan.latent]
            extra = block[:, plan.latent :].astype(F32)
            if side is core:
                lgain = lgain + extra[: plan.lrow] + extra[plan.lrow : 2 * plan.lrow]
            at_gain = 2 * plan.lrow
            ggain = ggain + extra[at_gain : at_gain + plan.grow] + extra[at_gain + plan.grow : at_gain + 2 * plan.grow]
    wide, low = plan.wcol // plan.spare, plan.ccol // plan.spare
    for b in range(n):
        for i in range(wide):
            m_s[b, :, i * plan.spare : (i + 1) * plan.spare] = ggain[b * wide + i : b * wide + i + 1, :]
        for i in range(low):
            l_s[b, :, i * plan.spare : (i + 1) * plan.spare] = lgain[b * low + i : b * low + i + 1, :]
    g_gain[...] = m_s[j]
    g_lg[...] = l_s[j]
    g_lat[...] = mm_tn(a_dl[...], a_n[...])
    g_out[...] = mm_tn(a_m[...], a_u[...])


def grouped(counts_in, refs):
    out, at = [], 0
    for count in counts_in:
        if count is None:
            out.append(refs[at])
            at += 1
        else:
            out.append(list(refs[at : at + count]))
            at += count
    return out


def kernel_call(body, groups, out_groups, scratch, flops, inputs=pltpu.VMEM):
    def flat(items):
        return [leaf for item in items for leaf in (item if isinstance(item, list) else [item])]

    counts = [len(g) if isinstance(g, list) else None for g in groups + out_groups] + [None] * len(scratch)

    def kernel(*refs):
        body(*grouped(counts, refs))

    outs = flat(out_groups)
    vmem = pl.BlockSpec(memory_space=pltpu.VMEM)
    ins = flat(groups)
    call = pl.pallas_call(
        kernel,
        in_specs=[pl.BlockSpec(memory_space=pltpu.SMEM)] + [pl.BlockSpec(memory_space=inputs)] * (len(ins) - 1),
        out_specs=[vmem] * len(outs),
        out_shape=outs,
        scratch_shapes=scratch,
        compiler_params=pltpu.CompilerParams(vmem_limit_bytes=20 << 20),
        cost_estimate=pl.CostEstimate(flops=flops, bytes_accessed=4 << 20, transcendentals=0),
    )
    got = call(*ins)
    result, at = [], 0
    for g in out_groups:
        if isinstance(g, list):
            result.append(list(got[at : at + len(g)]))
            at += len(g)
        else:
            result.append(got[at])
            at += 1
    return result


def flipped(value, axis, count, bit):
    return lax.ppermute(value, axis, [(i, i ^ bit) for i in range(count)])


def gathered(value, axis, count):
    blocks = {0: value}
    bit = count // 2
    while bit:
        found = sorted(blocks)
        blocks.update({k | bit: flipped(blocks[k], axis, count, bit) for k in found})
        bit //= 2
    return [blocks[k] for k in range(count)]


def handed(values, axis, count):
    return [values[0]] + [flipped(values[k], axis, count, k) for k in range(1, count)]


def token_shards(plan, saved, top_grad, gain, w_query, w_latent, compressed_gain, expand_weight, w_output):
    n, nt, rows = plan.n, plan.nt, plan.rows
    j = lax.axis_index("dp")
    t = lax.axis_index("tensor")
    section = lax.axis_index("pipe")
    is_top = (section == plan.n_pipe - 1).astype(jnp.int32)
    ranks = jnp.stack([j, t, is_top]).astype(jnp.int32)

    def shape(dims, kind=BF16):
        return jax.ShapeDtypeStruct(dims, kind)

    def pick(*refs):
        piece_body(plan, *refs)

    def stack(ranks, blocks, target, gain_ref, gain_s):
        for k, block in enumerate(blocks):
            target[k * (plan.part + 16) : (k + 1) * (plan.part + 16), :] = block[...]
            gain_s[ranks[0] ^ k] = block[plan.part : plan.part + 16, :].astype(F32)[:1]
        for b in range(n):
            gain_ref[:, b * plan.wcol : (b + 1) * plan.wcol] = gain_s[b]

    tall = plan.part + 16
    (piece,) = kernel_call(
        pick,
        [ranks, w_latent[0].T, gain, compressed_gain],
        [shape((tall, plan.wcol))],
        [pltpu.VMEM((1, plan.wcol), BF16), pltpu.VMEM((1, plan.ccol), BF16), pltpu.SemaphoreType.DMA((3,))],
        10**4,
        pltpu.HBM,
    )
    blocks = gathered(piece, "dp", n)
    stacked, gain_all = kernel_call(
        stack,
        [ranks, blocks],
        [shape((n * tall, plan.wcol)), shape((1, plan.width), F32)],
        [pltpu.VMEM((n, 1, plan.wcol), F32)],
        10**4,
    )
    lat = gathered(stacked, "tensor", nt)
    wq = gathered(w_query[0], "dp", n)
    wexp = gathered(expand_weight[0], "dp", n)
    wout = gathered(w_output[0], "dp", n)
    x = saved[0].reshape(rows, plan.width)
    top = top_grad.reshape(rows, plan.width)
    freq = 10000.0 ** (-np.arange(ROPE // 2) / (ROPE // 2))
    angle = np.tile(np.arange(plan.length)[:, None] * freq[None, :], (plan.micro, 1))
    cos, sin = np.cos(angle), np.sin(angle)
    table = jnp.asarray(np.concatenate([cos, cos, -sin, sin], axis=1), F32)

    def prepare(ranks, sources, targets, *rest):
        sems = rest[-1]
        moves = [pltpu.make_async_copy(a, b, sems.at[i]) for i, (a, b) in enumerate(zip(sources, targets))]
        for move in moves:
            move.start()
        for move in moves:
            move.wait()
        if len(rest) > 1:
            for start, at in share_rows(plan, lax.rem(ranks[1], 2)):
                rest[0][at, :] = targets[0][pl.ds(start, plan.share), :]

    def local(values, extra):
        shapes = [shape(v.shape, v.dtype) for v in values]
        sems = [pltpu.SemaphoreType.DMA((len(values),))]
        return kernel_call(prepare, [ranks, values], [shapes] + extra, sems, 10**4, pltpu.HBM)

    (x, wq[0], wexp[0], table), x_own = local([x, wq[0], wexp[0], table], [shape((plan.half, plan.width))])
    ((top, wout[0]),) = local([top, wout[0]], [])
    down = [(i, i - 1) for i in range(1, plan.n_pipe)]
    x_above = lax.ppermute(x_own, "pipe", down)
    gain_above = lax.ppermute(gain_all, "pipe", down)

    def forward(ranks, x, wq, lat, we, table, *outs):
        forward_body(plan, ranks, x, wq, lat, we, table, outs)

    sent, pay, v, p, chat, rc, gain32, cgain32, wlat = kernel_call(
        forward,
        [ranks, x, wq, lat, wexp, table],
        [
            [shape((plan.half, plan.wcol + plan.ccol))] * n,
            shape((rows, plan.pay)),
            shape((rows, plan.hcol)),
            shape((plan.heads, rows, rows), F32),
            shape((rows, plan.rank), F32),
            shape((rows, 1), F32),
            shape((1, plan.width), F32),
            shape((1, plan.rank), F32),
            shape((n, plan.latent, plan.wcol)),
        ],
        [
            pltpu.VMEM((n, 1, plan.wcol), F32),
            pltpu.VMEM((n, 1, plan.ccol), F32),
            pltpu.VMEM((n, rows, plan.wcol), BF16),
            pltpu.VMEM((n, rows, plan.ccol), BF16),
        ],
        5 * 10**8,
    )
    pieces = []
    for tick in range(plan.n_pipe):
        last = tick == plan.n_pipe - 1

        def backward(ranks, top, pieces, pay, v, p, chat, rc, cg, wq, wl, we, wo, table, *outs):
            outs = list(outs)
            if not last:
                outs[2:2] = [None, None]
            backward_body(plan, last, ranks, top, pieces, pay, v, p, chat, rc, cg, wq, wl, we, wo, table, outs)

        chunk = plan.chunk if last else plan.width
        out_groups = [[shape((plan.half, chunk))] * 2, shape((plan.half, plan.width))]
        if last:
            out_groups += [shape((rows, plan.tail)), [shape((plan.half, plan.wcol))] * n]
        got = kernel_call(
            backward,
            [ranks, top, pieces, pay, v, p, chat, rc, cgain32, wq, wlat, wexp, wout, table],
            out_groups,
            [
                pltpu.VMEM((rows, plan.width), BF16),
                pltpu.VMEM((n, rows, plan.wcol), BF16),
                pltpu.VMEM((n, rows, plan.ccol), F32),
                pltpu.VMEM((n, rows, plan.wcol), BF16),
                pltpu.VMEM((rows, plan.latent + plan.spare), BF16),
            ],
            10**9,
        )
        (kept, given), up_own = got[0], got[1]
        chip = kept + flipped(given, "tensor", nt, 1)
        if not last:
            sums = []
            for k in range(nt // 2):
                pairs = [(s * nt + i, r * nt + (i + 2 * k) % nt) for s, r in down for i in range(nt)]
                sums.append(lax.ppermute(chip, ("pipe", "tensor"), pairs))
            above = up_own if tick == 0 else lax.ppermute(up_own, "pipe", down)
            norm_in = [ranks, sums, above, x_above, gain_above]
            norm_out = [shape((plan.half, plan.width))]
        else:
            sums = [chip]
            for k in range(1, nt // 2):
                pairs = [(i, (i + 2 * k) % nt) for i in range(nt)]
                sums.append(lax.ppermute(chip, "tensor", pairs))
            tail, ups = got[2], got[3]
            norm_in = [ranks, sums, up_own, x_own, gain32]
            norm_out = [shape((plan.own, plan.width)), shape((plan.half, plan.latent + plan.spare))]

        def norm(ranks, sums, up_own, x_own, gain32, *rest):
            dx, dl, dx_s = rest if last else (rest[0], None, rest[1])
            norm_body(plan, last, ranks, sums, up_own, x_own, gain32, dx, dl, dx_s)

        got = kernel_call(norm, norm_in, norm_out, [pltpu.VMEM((plan.half, plan.width), BF16)], 10**6)
        dx = got[0]
        if not last:
            pieces = [dx, flipped(dx, "tensor", nt, 1)]
    dl_own = gathered(got[1], "dp", n)
    dl_other = [flipped(block, "tensor", nt, 1) for block in dl_own]
    sent = handed(sent, "dp", n)
    sent_o = [flipped(block, "tensor", nt, 1) for block in sent]
    pays = gathered(pay, "dp", n)
    tails = gathered(tail, "dp", n)
    ups = handed(ups, "dp", n)
    ups_o = [flipped(block, "tensor", nt, 1) for block in ups]

    def gradients(ranks, sent, sent_o, pays, tails, table, *outs):
        gradient_body(plan, ranks, sent, sent_o, pays, tails, table, outs)

    def latent_gradients(ranks, sent, sent_o, pays, ups, ups_o, dl_own, dl_other, *outs):
        latent_gradient_body(plan, ranks, sent, sent_o, pays, ups, ups_o, dl_own, dl_other, outs)

    every = n * rows
    g_q, g_exp = kernel_call(
        gradients,
        [ranks, sent, sent_o, pays, tails, table],
        [shape((plan.wcol, plan.qcol), F32), shape((plan.ccol, plan.heads * (NOPE + VDIM)), F32)],
        [
            pltpu.VMEM((every, plan.wcol), BF16),
            pltpu.VMEM((every, plan.ccol), BF16),
            pltpu.VMEM((every, plan.qcol), BF16),
            pltpu.VMEM((every, plan.heads * (NOPE + VDIM)), BF16),
        ],
        10**9,
    )
    g_gain, g_lat, g_lg, g_out = kernel_call(
        latent_gradients,
        [ranks, sent, sent_o, pays, ups, ups_o, dl_own, dl_other],
        [
            shape((1, plan.wcol), F32),
            shape((plan.latent, plan.wcol), F32),
            shape((1, plan.ccol), F32),
            shape((plan.hcol, plan.wcol), F32),
        ],
        [
            pltpu.VMEM((every, plan.wcol), BF16),
            pltpu.VMEM((every, plan.hcol), BF16),
            pltpu.VMEM((every, plan.wcol), BF16),
            pltpu.VMEM((every, plan.latent), BF16),
            pltpu.VMEM((n, 1, plan.wcol), F32),
            pltpu.VMEM((n, 1, plan.ccol), F32),
        ],
        10**9,
    )
    results = dx.reshape(plan.micro, plan.share, plan.width)
    return results[None], g_gain, g_q[None], g_lat.T[None], g_lg, g_exp[None], g_out[None]


def shards(saved, top_grad, gain, w_query, w_latent, compressed_gain, expand_weight, w_output):
    args = (saved, top_grad, gain, w_query, w_latent, compressed_gain, expand_weight, w_output)
    sizes = [lax.axis_size(axis) for axis in ("pipe", "dp", "tensor")]
    plan = Plan(saved, w_query, w_latent, expand_weight, *sizes)
    if plan.fits():
        return token_shards(plan, *args)
    return plain_shards(*args)


def solution(mesh):
    in_specs = (
        P("pipe", None, "dp", None),
        P(None, "dp", None),
        P("pipe", "dp"),
        P("pipe", "dp", "tensor"),
        P("pipe", "dp", None),
        P("pipe", "dp"),
        P("pipe", "dp", "tensor"),
        P("pipe", "tensor", "dp"),
    )
    out_specs = (
        P("pipe", None, ("dp", "tensor"), None),
        P("pipe", "dp"),
        P("pipe", "dp", "tensor"),
        P("pipe", "dp", None),
        P("pipe", "dp"),
        P("pipe", "dp", "tensor"),
        P("pipe", "tensor", "dp"),
    )
    return jax.shard_map(shards, mesh=mesh, in_specs=in_specs, out_specs=out_specs, check_vma=False)
```
